256 devices in a mesh: space: 16 (over z_hi, x, core), freq: 16 (over y, z_lo).
Axes of the slice: x: 4, y: 4, z: 8 (z_hi: 2, z_lo: 4; z = z_hi * 4 + z_lo), core: 2. Of those that a mesh axis runs over, the one named last changes fastest.
Arguments:
- spectrum: float32 [32, 36, 512, 256], P('freq', None, 'space'), may hold values from 0.05 to 2
- land_sea: int32 [512, 256], P('space'), may hold values 0 or 1
- courant: float32 [32], P('freq'), may hold values from 0.2 to 0.65
- refract: float32 [32], P('freq'), may hold values from 0.2 to 0.9
- depth_dx: float32 [512, 256], P('space'), may hold values from -0.5 to 0.5
- depth_dy: float32 [512, 256], P('space'), may hold values from -0.5 to 0.5
- w_in: bfloat16 [1152, 2048], P(None, 'freq'), may hold values from -0.1875 to 0.1875
- w_out: bfloat16 [2048, 1152], P('freq'), may hold values from -0.125 to 0.125
Outputs:
- spectrum_out: float32 [32, 36, 512, 256], P('freq', None, 'space')
The draws below stay inside these ranges and needn't reach their ends.
All inputs are finite; a program needn't handle non-finite values. No bound on the sum of `land_sea` on one device may be relied on, other than what follows from the above.
Results may differ from the reference program's by a relative error of at most 0.003.
Values may be sent and summed in bfloat16 or wider, within the bound.
A program may use at most 128 MiB of HBM per device.

```python
import math
import jax
import jax.numpy as jnp
from jax import lax

F = 32
DIRS = 36
HIDDEN_SIZE = 2048
PX = 32
PY = 256
STEPS = 2
CHAN = 1152
NX = 512


def touch_ends(array, rng, low, top_value):
    extent = array.shape
    index_at = [jax.random.randint(jax.random.fold_in(rng, axis), (), 0, extent[axis]) for axis in range(len(extent))]
    array = array.at[tuple(index_at)].set(low)
    longest = extent.index(max(extent))
    index_at[longest] = (index_at[longest] + 1) % extent[longest]
    return array.at[tuple(index_at)].set(top_value)


def steps_of(own_key, dims, pieces, least, high):
    factor_of, own = 1.0, jax.random.fold_in(own_key, 6)
    for axis_at, parts in pieces:
        heights = jnp.exp(jax.random.uniform(jax.random.fold_in(own, axis_at), (parts,), jnp.float32, least / len(pieces), high / len(pieces)))
        factor_of = factor_of * jnp.repeat(heights, dims[axis_at] // parts).reshape([-1 if axis == axis_at else 1 for axis in range(len(dims))])
    return factor_of


def bell_draw(stream_key, shape, width, reach, shards=(), kind=jnp.bfloat16):
    array = jax.random.normal(stream_key, shape, jnp.float32) * width
    if len(shards) > 0:
        array = steps_of(stream_key, shape, shards, -0.22, 0.18) * array
    return jnp.clip(array, min=-reach, max=reach).astype(kind)


def setup_inputs(seed: int = 0) -> dict:
    splits = jax.random.split(jax.random.key(seed), 9)
    spectrum = jnp.clip(jnp.exp(math.log(2.0) - 3.6888794 * jax.random.uniform(splits[0], (F, DIRS, NX, PY), jnp.float32) ** steps_of(splits[0], (F, DIRS, NX, PY), ((0, 16), (2, 16)), -0.2, 0.2)), 0.05, 2.0)
    land_sea = touch_ends((jax.random.randint(splits[1], (NX, PY), 0, 8) < 7).astype(jnp.int32), jax.random.fold_in(splits[1], 1), 0, 1)
    courant = jnp.clip(0.2 + 0.45 * jax.random.uniform(splits[2], (F,), jnp.float32) ** steps_of(splits[2], (F,), ((0, 16),), -0.2, 0.2), 0.2, 0.65)
    refract = jnp.clip(0.2 + 0.7 * jax.random.uniform(splits[3], (F,), jnp.float32) ** steps_of(splits[3], (F,), ((0, 16),), -0.2, 0.2), 0.2, 0.9)
    depth_dx = jnp.clip(jax.random.uniform(splits[4], (NX, PY), jnp.float32, -0.5, 0.5) * steps_of(splits[4], (NX, PY), ((0, 16),), -0.4, 0.0), -0.5, 0.5)
    depth_dy = jnp.clip(jax.random.uniform(splits[5], (NX, PY), jnp.float32, -0.5, 0.5) * steps_of(splits[5], (NX, PY), ((0, 16),), -0.4, 0.0), -0.5, 0.5)
    w_in = bell_draw(splits[6], (CHAN, HIDDEN_SIZE), CHAN ** -0.5, 0.1875, ((1, 16),))
    w_out = bell_draw(splits[7], (HIDDEN_SIZE, CHAN), HIDDEN_SIZE ** -0.5, 0.125, ((0, 16),))
    return dict(spectrum=spectrum, land_sea=land_sea, courant=courant, refract=refract, depth_dx=depth_dx, depth_dy=depth_dy, w_in=w_in, w_out=w_out)


step_scale = 0.5
epsilon = 1e-6


def direction_tables():
    angles = (jnp.arange(DIRS, dtype=jnp.float32) + 0.5) * (2.0 * math.pi / DIRS)
    return jnp.cos(angles), jnp.sin(angles)


def transport(padded, courant, refract, depth_dx, depth_dy, seamask):
    cosine, sine_dir = direction_tables()
    speed_x = courant[:, None] * cosine[None, :]
    speed_y = courant[:, None] * sine_dir[None, :]
    pos_x = jnp.maximum(speed_x, 0.0)[:, :, None, None]
    neg_x = jnp.maximum(-speed_x, 0.0)[:, :, None, None]
    pos_y = jnp.maximum(speed_y, 0.0)[:, :, None, None]
    neg_y = jnp.maximum(-speed_y, 0.0)[:, :, None, None]
    center = padded[:, :, 1:-1, 1:-1]
    keeping = 1.0 - jnp.abs(speed_x)[:, :, None, None] - jnp.abs(speed_y)[:, :, None, None]
    shifted = center * keeping + pos_x * padded[:, :, :-2, 1:-1] + neg_x * padded[:, :, 2:, 1:-1]
    shifted = shifted + pos_y * padded[:, :, 1:-1, :-2] + neg_y * padded[:, :, 1:-1, 2:]
    turn_rate = refract[:, None, None, None] * (sine_dir[None, :, None, None] * depth_dx[None, None]
                                                - cosine[None, :, None, None] * depth_dy[None, None])
    turn_pos = jnp.maximum(turn_rate, 0.0)
    turn_neg = jnp.maximum(-turn_rate, 0.0)
    turned = shifted * (1.0 - jnp.abs(turn_rate)) + jnp.roll(turn_pos * shifted, 1, axis=1)
    turned = turned + jnp.roll(turn_neg * shifted, -1, axis=1)
    return turned * seamask[None, None]


def interact(block, w_in, w_out):
    contract = (((0,), (0,)), ((), ()))
    energy_mean = jnp.mean(block, axis=0) + epsilon
    scaled = (block / energy_mean[None]).astype(jnp.bfloat16)
    preact = lax.dot_general(w_in, scaled, contract, preferred_element_type=jnp.float32)
    hidden = jax.nn.gelu(preact).astype(jnp.bfloat16)
    source = lax.dot_general(w_out, hidden, contract, preferred_element_type=jnp.float32).astype(jnp.bfloat16)
    return block * jnp.exp(step_scale * jnp.tanh(source.astype(jnp.float32)))


def reference(spectrum, land_sea, courant, refract, depth_dx, depth_dy, w_in, w_out):
    seamask = land_sea.astype(jnp.float32)
    field = spectrum
    blocks_count = NX // PX

    def one_frequency(inputs):
        layer, speed, bending = inputs
        padded = jnp.pad(layer[None], ((0, 0), (0, 0), (1, 1), (1, 1)))
        return transport(padded, speed[None], bending[None], depth_dx, depth_dy, seamask)[0]

    def one_block(block):
        return interact(block, w_in, w_out)

    for repeat in range(STEPS):
        field = lax.map(one_frequency, (field, courant, refract))
        blocks = field.reshape(CHAN, blocks_count, PX * PY).transpose(1, 0, 2)
        updated = lax.map(one_block, blocks)
        field = updated.transpose(1, 0, 2).reshape(F, DIRS, NX, PY)
    return field
```

```python
import math

import jax
import jax.numpy as jnp
from jax import lax
from jax.experimental import pallas as pl
from jax.experimental.pallas import tpu as pltpu
from jax.sharding import PartitionSpec as P

DIRS = 36
MESH = pl.DeviceIdType.MESH

step_scale = 0.5
epsilon = 1e-06

TOP_T1 = 2.45
TOP_E1 = 4.06
TOP_E2 = 8.2
LEVELS = 65535.0
HALF = 32768.0


def encode(value, top):
    level = jnp.minimum(value * (LEVELS / top) + 0.5, LEVELS)
    return (level.astype(jnp.int32) - 32768).astype(jnp.int16)


def decode(code, top):
    return (code.astype(jnp.int32).astype(jnp.float32) + HALF) * (top / LEVELS)


def freq_of(j):
    zl = j // 4
    yy = j % 4
    return (yy + (zl % 2) * (3 - 2 * yy)) * 4 + zl


def place_of(f):
    y = f // 4
    zl = f % 4
    return zl * 4 + y + (zl % 2) * (3 - 2 * y)


def coefficients(table, cosine, sine):
    first = lax.broadcasted_iota(jnp.int32, cosine.shape, 0) < DIRS
    courant = jnp.where(first, table[0:1], table[1:2])
    refract = jnp.where(first, table[2:3], table[3:4])
    speed_x = courant * cosine
    speed_y = courant * sine
    pos_x = jnp.maximum(speed_x, 0.0)
    pos_y = jnp.maximum(speed_y, 0.0)
    keep = 1.0 - jnp.abs(speed_x) - jnp.abs(speed_y)
    return keep, pos_x, pos_x - speed_x, pos_y, pos_y - speed_y, refract * sine, refract * cosine


def transport_row(before, center, after, coef, dx, dy, sea):
    keep, pos_x, neg_x, pos_y, neg_y, turn_x, turn_y = coef
    rows, cols = center.shape
    lane = lax.broadcasted_iota(jnp.int32, center.shape, 1)
    west = jnp.where(lane == 0, 0.0, pltpu.roll(center, 1, 1))
    east = jnp.where(lane == cols - 1, 0.0, pltpu.roll(center, cols - 1, 1))
    shifted = center * keep + pos_x * before + neg_x * after + pos_y * west + neg_y * east
    turning = (turn_x * dx - turn_y * dy) * shifted
    moved_up = jnp.maximum(turning, 0.0)
    moved_down = jnp.maximum(-turning, 0.0)
    d = lax.broadcasted_iota(jnp.int32, center.shape, 0)
    lower = jnp.where((d == 0) | (d == DIRS), pltpu.roll(moved_up, DIRS + 1, 0), pltpu.roll(moved_up, 1, 0))
    upper = jnp.where(
        (d == DIRS - 1) | (d == rows - 1),
        pltpu.roll(moved_down, DIRS - 1, 0),
        pltpu.roll(moved_down, rows - 1, 0),
    )
    return (shifted - jnp.abs(turning) + lower + upper) * sea


def gelu(x):
    return 0.5 * x * (1.0 + jnp.tanh(math.sqrt(2.0 / math.pi) * (x + 0.044715 * x * x * x)))


def kernel(
    field, dx, dy, sea, cos_ref, sin_ref, own_table, own_w, out,
    weights, codes1, got1, codes2, got2, table, edge_out, edge_in, energy, moved, x_buf, h_buf, s_buf, coef_buf,
    z_send, z_recv, y_send, y_recv, x_send, x_recv, d_send, d_recv, a_send, a_recv, t_send, t_recv,
    e_send, e_recv, b_send, b_recv, local_sem,
):
    s = lax.axis_index("space")
    f = lax.axis_index("freq")
    core = s % 2
    x = (s // 2) % 4
    base = (s // 8) * 8
    y = f // 4
    zl = f % 4
    j = place_of(f)
    chans = field.shape[1]
    cols = field.shape[2]
    groups = 16

    def at_freq(g):
        return {"space": s, "freq": g}

    def at_x(step):
        return {"space": base + ((x + step) % 4) * 2 + core, "freq": f}

    partner = {"space": s + 1 - 2 * core, "freq": f}
    has_up = jnp.logical_or(j > 0, s > 0)
    has_down = jnp.logical_or(j < 15, s < 15)
    up = {"space": jnp.where(j > 0, s, jnp.maximum(s - 1, 0)), "freq": freq_of((j + 15) % 16)}
    down = {"space": jnp.where(j < 15, s, jnp.minimum(s + 1, 15)), "freq": freq_of((j + 1) % 16)}

    barrier = pltpu.get_barrier_semaphore()
    for k in range(1, groups):
        pl.semaphore_signal(barrier, inc=1, device_id=at_freq((f + k) % 16), device_id_type=MESH)
    pl.semaphore_signal(barrier, inc=1, device_id=at_x(1), device_id_type=MESH)
    pl.semaphore_signal(barrier, inc=1, device_id=at_x(3), device_id_type=MESH)
    pl.semaphore_signal(barrier, inc=1, device_id=partner, device_id_type=MESH)
    over_top = jnp.logical_and(j == 0, s > 0)
    over_bottom = jnp.logical_and(j == 15, s < 15)

    @pl.when(over_top)
    def _():
        pl.semaphore_signal(barrier, inc=1, device_id=up, device_id_type=MESH)

    @pl.when(over_bottom)
    def _():
        pl.semaphore_signal(barrier, inc=1, device_id=down, device_id_type=MESH)

    pl.semaphore_wait(barrier, 18 + over_top.astype(jnp.int32) + over_bottom.astype(jnp.int32))

    def remote(src, dst, send, recv, target):
        return pltpu.make_async_remote_copy(
            src_ref=src, dst_ref=dst, send_sem=send, recv_sem=recv, device_id=target, device_id_type=MESH
        )

    def quarter(q):
        return pl.ds(pl.multiple_of(q * 32, 32), 32)

    own_quarter = weights.at[core, f, :, quarter(x), :]
    place = pltpu.make_async_copy(own_w.at[core, :, quarter(x), :], own_quarter, local_sem.at[0])
    place.start()
    place.wait()
    z_copies = []
    for k in range(1, 4):
        c = remote(own_quarter, own_quarter, z_send.at[k - 1], z_recv.at[k - 1], at_freq(y * 4 + (zl + k) % 4))
        c.start()
        z_copies.append(c)
    table[f] = own_table[...]
    t_copies = []
    for k in range(1, groups):
        c = remote(own_table, table.at[f], t_send.at[k], t_recv.at[k], at_freq((f + k) % 16))
        c.start()
        t_copies.append(c)

    def y_block(r, first=0, count=4, q=x):
        return weights.at[core, pl.ds(r * 4 + first, count), :, quarter(q), :]

    y_right, y_left = at_freq(((y + 1) % 4) * 4 + zl), at_freq(((y + 3) % 4) * 4 + zl)
    order = [y, (y + 3) % 4, (y + 1) % 4, (y + 2) % 4]
    xs = [x, (x + 3) % 4, (x + 1) % 4, (x + 2) % 4]
    y_copies, x_copies, d_copies = {}, {}, {}

    def go(where, key, copy):
        copy.start()
        where[key] = copy

    def spread(b):
        r = order[b]
        block = y_block(r)
        go(x_copies, (b, 0), remote(block, block, x_send.at[b, 0], x_recv.at[b, 0], at_x(1)))
        go(x_copies, (b, 1), remote(block, block, x_send.at[b, 1], x_recv.at[b, 1], at_x(3)))
        share(b, 0)

    def share(b, k):
        block = y_block(order[b], q=xs[k])
        go(d_copies, (b, k), remote(block, block, d_send.at[b, k], d_recv.at[b, k], partner))

    def weights_1():
        for c in z_copies:
            c.wait_recv()
        own = y_block(y)
        go(y_copies, 0, remote(own, own, y_send.at[0], y_recv.at[0], y_right))
        go(y_copies, 1, remote(own, own, y_send.at[1], y_recv.at[1], y_left))
        spread(0)

    def weights_2():
        y_copies[0].wait_recv()
        part = y_block(order[1], 0, 2)
        go(y_copies, 2, remote(part, part, y_send.at[2], y_recv.at[2], y_right))
        spread(1)

    def weights_3():
        y_copies[1].wait_recv()
        part = y_block(order[2], 2, 2)
        go(y_copies, 3, remote(part, part, y_send.at[3], y_recv.at[3], y_left))
        spread(2)

    def weights_4():
        y_copies[2].wait_recv()
        y_copies[3].wait_recv()
        spread(3)

    def weights_5(b):
        x_copies[b, 0].wait_recv()
        part = y_block(order[b], 0, 2, xs[1])
        go(x_copies, (b, 2), remote(part, part, x_send.at[b, 2], x_recv.at[b, 2], at_x(1)))
        share(b, 1)
        x_copies[b, 1].wait_recv()
        part = y_block(order[b], 2, 2, xs[2])
        go(x_copies, (b, 3), remote(part, part, x_send.at[b, 3], x_recv.at[b, 3], at_x(3)))
        share(b, 2)

    def weights_6(b):
        x_copies[b, 2].wait_recv()
        x_copies[b, 3].wait_recv()
        share(b, 3)

    coef = coefficients(own_table[...], cos_ref[...], sin_ref[...])
    for i, c in enumerate(coef):
        coef_buf[i] = c

    def first_rows(k, carry):
        jj = (j + k) % 16
        for r in range(2):
            row = jj * 2 + r
            value = transport_row(
                field[row], field[row + 1], field[row + 2], [coef_buf[i] for i in range(7)], dx[row], dy[row], sea[row]
            )
            codes1[jj, r] = encode(value, TOP_T1)
        return carry

    a_copies = []
    hooks = {3: weights_1, 7: weights_2, 9: weights_3, 12: weights_4}

    def send_rows(k):
        jj = (j + k) % 16
        c = remote(codes1.at[jj], got1.at[f], a_send.at[k], a_recv.at[k], at_freq(freq_of(jj)))
        c.start()
        a_copies.append(c)

    def first_and_send(k, carry):
        first_rows(k, carry)
        jj = (j + k) % 16
        remote(codes1.at[jj], got1.at[f], a_send.at[k], a_recv.at[jj * 0 + k], at_freq(freq_of(jj))).start()
        return carry

    bounds = [1, 4, 7, 10, 13, 16]
    steps = [weights_1, weights_2, weights_3, weights_4, None]
    for n in range(5):
        lax.fori_loop(bounds[n], bounds[n + 1], first_and_send, 0)
        if steps[n] is not None:
            steps[n]()
    first_rows(0, 0)
    mine = pltpu.make_async_copy(codes1.at[j], got1.at[f], local_sem.at[0])
    mine.start()
    mine.wait()
    for b in range(4):
        weights_5(b)

    def await_rows(k, carry):
        g = freq_of((j + 16 - k) % 16)
        remote(codes1.at[0], got1.at[g], a_send.at[k], a_recv.at[k], at_freq(g)).wait_recv()
        return carry

    lax.fori_loop(1, 16, await_rows, 0)
    for b in range(4):
        weights_6(b)
    for c in d_copies.values():
        c.wait_recv()

    def network():
        def first_layer(i, carry):
            lhs = jnp.concatenate(
                [
                    jnp.concatenate([weights[0, i * 4 + q, k] for k in range(9)], axis=1)
                    for q in range(4)
                ],
                axis=0,
            )
            pre = jnp.dot(lhs, x_buf[...], preferred_element_type=jnp.float32)
            h_buf[pl.ds(pl.multiple_of(i * 512, 512), 512), :] = gelu(pre).astype(jnp.bfloat16)
            return carry

        lax.fori_loop(0, 4, first_layer, 0)

        def second_layer(i, carry):
            lhs = jnp.concatenate(
                [
                    jnp.concatenate([weights[1, g, i * 3 + k] for g in range(16)], axis=1)
                    for k in range(3)
                ],
                axis=0,
            )
            s_buf[pl.ds(pl.multiple_of(i * 384, 384), 384), :] = jnp.dot(
                lhs, h_buf[...], preferred_element_type=jnp.float32
            )
            return carry

        lax.fori_loop(0, 3, second_layer, 0)

    def scale_into_x(total):
        mean = jnp.sum(total, axis=0, keepdims=True) * (1.0 / 1152.0) + epsilon
        inverse = 1.0 / mean

        def pair(p, carry):
            both = jnp.concatenate([moved[p * 2], moved[p * 2 + 1]], axis=0) * inverse
            x_buf[pl.ds(pl.multiple_of(p * 144, 144), 144), :] = both.astype(jnp.bfloat16)
            return carry

        lax.fori_loop(0, 8, pair, 0)

    def growth(g):
        return jnp.exp(step_scale * jnp.tanh(s_buf[pl.ds(pl.multiple_of(g * 72, 8), 72), :]))

    zeros = jnp.zeros((chans, cols), jnp.float32)
    edge_copies = []
    for r in range(2):

        def load(g, total):
            value = decode(got1[g, r], TOP_T1)
            moved[g] = value
            return total + value

        scale_into_x(lax.fori_loop(0, groups, load, zeros))
        network()

        def update(g, carry):
            value = moved[g] * growth(g)
            energy[g, r + 1] = value
            edge_out[r, g] = encode(value, TOP_E1)
            return carry

        lax.fori_loop(0, groups, update, 0)
        c = remote(edge_out.at[r], edge_in.at[1 - r], e_send.at[r], e_recv.at[1 - r], up if r == 0 else down)
        edge_copies.append(c)
        pl.when(has_up if r == 0 else has_down)(c.start)

    for k in range(1, groups):
        t_copies[k - 1].wait_recv()

    @pl.when(has_up)
    def _():
        edge_copies[1].wait_recv()

        def fill(g, carry):
            energy[g, 0] = decode(edge_in[0, g], TOP_E1)
            return carry

        lax.fori_loop(0, groups, fill, 0)

    @pl.when(jnp.logical_not(has_up))
    def _():
        def fill(g, carry):
            energy[g, 0] = zeros
            return carry

        lax.fori_loop(0, groups, fill, 0)

    @pl.when(has_down)
    def _():
        edge_copies[0].wait_recv()

        def fill(g, carry):
            energy[g, 3] = decode(edge_in[1, g], TOP_E1)
            return carry

        lax.fori_loop(0, groups, fill, 0)

    @pl.when(jnp.logical_not(has_down))
    def _():
        def fill(g, carry):
            energy[g, 3] = zeros
            return carry

        lax.fori_loop(0, groups, fill, 0)

    for r in range(2):
        row = j * 2 + r

        def second(g, total):
            coef = coefficients(table[g], cos_ref[...], sin_ref[...])
            value = transport_row(energy[g, r], energy[g, r + 1], energy[g, r + 2], coef, dx[row], dy[row], sea[row])
            moved[g] = value
            return total + value

        scale_into_x(lax.fori_loop(0, groups, second, zeros))
        network()

        def finish(k, carry):
            g = (f + k) % 16
            codes2[g, r] = encode(moved[g] * growth(g), TOP_E2)
            return carry

        def finish_and_send(k, carry):
            finish(k, carry)
            g = (f + k) % 16
            remote(codes2.at[g, r], got2.at[j, r], b_send.at[r, k], b_recv.at[r, k], at_freq(g)).start()
            return carry

        lax.fori_loop(1, groups, finish_and_send, 0)
        finish(0, 0)

    own_back = pltpu.make_async_copy(codes2.at[f], got2.at[j], local_sem.at[0])
    own_back.start()
    own_back.wait()

    def await_back(k, carry):
        g = (f + 16 - k) % 16
        for r in range(2):
            remote(codes2.at[0, 0], got2.at[place_of(g), r], b_send.at[r, k], b_recv.at[r, k], at_freq(g)).wait_recv()
        return carry

    lax.fori_loop(1, groups, await_back, 0)

    def put(row, carry):
        out[row * 2] = got2[row, 0]
        out[row * 2 + 1] = got2[row, 1]
        return carry

    lax.fori_loop(0, groups, put, 0)

    for c in z_copies + t_copies + list(y_copies.values()) + list(x_copies.values()) + list(d_copies.values()):
        c.wait_send()

    def sent(k, carry):
        remote(codes1.at[0], got1.at[0], a_send.at[k], a_recv.at[k], partner).wait_send()
        for r in range(2):
            remote(codes2.at[0, 0], got2.at[0, 0], b_send.at[r, k], b_recv.at[r, k], partner).wait_send()
        return carry

    lax.fori_loop(1, groups, sent, 0)
    for r in range(2):
        pl.when(has_up if r == 0 else has_down)(edge_copies[r].wait_send)


def direction_tables():
    angles = (jnp.arange(DIRS, dtype=jnp.float32) + 0.5) * (2.0 * math.pi / DIRS)
    return (jnp.cos(angles), jnp.sin(angles))


def body(spectrum, land_sea, courant, refract, depth_dx, depth_dy, w_in, w_out):
    freqs, dirs, rows, cols = spectrum.shape
    chans = freqs * dirs
    count = lax.axis_size("space")
    forward = [(i, i + 1) for i in range(count - 1)]
    backward = [(b, a) for a, b in forward]
    low = lax.ppermute(spectrum[:, :, rows - 1 :], "space", forward)
    high = lax.ppermute(spectrum[:, :, :1], "space", backward)
    padded = jnp.concatenate([low, spectrum, high], axis=2).reshape(chans, rows + 2, cols)
    field = jnp.transpose(padded, (1, 0, 2))
    cosine, sine = direction_tables()
    cos_table = jnp.broadcast_to(jnp.tile(cosine, freqs)[:, None], (chans, cols))
    sin_table = jnp.broadcast_to(jnp.tile(sine, freqs)[:, None], (chans, cols))
    own_table = jnp.concatenate([courant, refract, jnp.zeros((4,), jnp.float32)])
    own_table = jnp.broadcast_to(own_table[:, None], (8, cols))
    first = jnp.transpose(w_in.reshape(9, 128, 128), (0, 2, 1))
    second = jnp.transpose(w_out.reshape(128, 9, 128), (1, 2, 0))
    own_w = jnp.stack([first, second])

    def line(a):
        return a.astype(jnp.float32).reshape(rows, 1, cols)

    vmem = pl.BlockSpec(memory_space=pltpu.VMEM)
    dma = pltpu.SemaphoreType.DMA
    i16, f32, b16 = jnp.int16, jnp.float32, jnp.bfloat16
    back = pl.pallas_call(
        kernel,
        out_shape=jax.ShapeDtypeStruct((rows, chans, cols), i16),
        in_specs=[vmem] * 8,
        out_specs=vmem,
        scratch_shapes=[
            pltpu.VMEM((2, 16, 9, 128, 128), b16),
            pltpu.VMEM((16, 2, chans, cols), i16),
            pltpu.VMEM((16, 2, chans, cols), i16),
            pltpu.VMEM((16, 2, chans, cols), i16),
            pltpu.VMEM((16, 2, chans, cols), i16),
            pltpu.VMEM((16, 8, cols), f32),
            pltpu.VMEM((2, 16, chans, cols), i16),
            pltpu.VMEM((2, 16, chans, cols), i16),
            pltpu.VMEM((16, 4, chans, cols), f32),
            pltpu.VMEM((16, chans, cols), f32),
            pltpu.VMEM((16 * chans, cols), b16),
            pltpu.VMEM((2048, cols), b16),
            pltpu.VMEM((16 * chans, cols), f32),
            pltpu.VMEM((7, chans, cols), f32),
            dma((3,)), dma((3,)), dma((4,)), dma((4,)), dma((4, 4)), dma((4, 4)), dma((4, 4)), dma((4, 4)),
            dma((16,)), dma((16,)), dma((16,)), dma((16,)), dma((2,)), dma((2,)), dma((2, 16)), dma((2, 16)),
            dma((1,)),
        ],
        compiler_params=pltpu.CompilerParams(
            collective_id=0, has_side_effects=True, vmem_limit_bytes=60 * 1024 * 1024
        ),
    )(field, line(depth_dx), line(depth_dy), line(land_sea), cos_table, sin_table, own_table, own_w)
    result = (jnp.transpose(back, (1, 0, 2)).astype(jnp.float32) + HALF) * (TOP_E2 / LEVELS)
    return result.reshape(freqs, dirs, rows, cols)


def solution(mesh):
    placed = (
        P("freq", None, "space", None),
        P("space", None),
        P("freq"),
        P("freq"),
        P("space", None),
        P("space", None),
        P(None, "freq"),
        P("freq", None),
    )
    return jax.shard_map(
        body, mesh=mesh, in_specs=placed, out_specs=P("freq", None, "space", None), check_vma=False
    )
```

```python
import math

import jax
import jax.numpy as jnp
import numpy as np
from jax import lax
from jax.experimental import pallas as pl
from jax.experimental.pallas import tpu as pltpu
from jax.sharding import PartitionSpec as P

DIRS = 36
MESH = pl.DeviceIdType.MESH

step_scale = 0.5
epsilon = 1e-06

TOP_T1 = 2.45
TOP_E1 = 4.06
TOP_E2 = 8.2
LEVELS = 65535.0
HALF = 32768.0


def encode(value, top):
    level = jnp.minimum(value * (LEVELS / top) + 0.5, LEVELS)
    return (level.astype(jnp.int32) - 32768).astype(jnp.int16)


def decode(code, top):
    return (code.astype(jnp.int32).astype(jnp.float32) + HALF) * (top / LEVELS)


def freq_of(rb, cb):
    high = rb // 4
    yy = rb % 4
    return (yy + high * (3 - 2 * yy)) * 4 + high * 2 + cb


def block_of(f):
    y = f // 4
    zl = f % 4
    high = zl // 2
    return high * 4 + y + high * (3 - 2 * y), zl % 2


def coefficients(table, cosine, sine):
    first = lax.broadcasted_iota(jnp.int32, cosine.shape, 0) < DIRS
    courant = jnp.where(first, table[0:1], table[1:2])
    refract = jnp.where(first, table[2:3], table[3:4])
    speed_x = courant * cosine
    speed_y = courant * sine
    pos_x = jnp.maximum(speed_x, 0.0)
    pos_y = jnp.maximum(speed_y, 0.0)
    keep = 1.0 - jnp.abs(speed_x) - jnp.abs(speed_y)
    return keep, pos_x, pos_x - speed_x, pos_y, pos_y - speed_y, refract * sine, refract * cosine


def transport_row(before, center, after, west_edge, east_edge, coef, dx, dy, sea):
    keep, pos_x, neg_x, pos_y, neg_y, turn_x, turn_y = coef
    rows, cols = center.shape
    lane = lax.broadcasted_iota(jnp.int32, center.shape, 1)
    west = jnp.where(lane == 0, west_edge, pltpu.roll(center, 1, 1))
    east = jnp.where(lane == cols - 1, east_edge, pltpu.roll(center, cols - 1, 1))
    shifted = center * keep + pos_x * before + neg_x * after + pos_y * west + neg_y * east
    turning = (turn_x * dx - turn_y * dy) * shifted
    moved_up = jnp.maximum(turning, 0.0)
    moved_down = jnp.maximum(-turning, 0.0)
    d = lax.broadcasted_iota(jnp.int32, center.shape, 0)
    lower = jnp.where((d == 0) | (d == DIRS), pltpu.roll(moved_up, DIRS + 1, 0), pltpu.roll(moved_up, 1, 0))
    upper = jnp.where(
        (d == DIRS - 1) | (d == rows - 1),
        pltpu.roll(moved_down, DIRS - 1, 0),
        pltpu.roll(moved_down, rows - 1, 0),
    )
    return (shifted - jnp.abs(turning) + lower + upper) * sea


def gelu(x):
    return 0.5 * x * (1.0 + jnp.tanh(math.sqrt(2.0 / math.pi) * (x + 0.044715 * x * x * x)))


def kernel(
    spectrum, dx, dy, land, courant, refract, cos_ref, sin_ref, w_in, w_out, out,
    field, own_table, own_w, weights, codes1, got1, codes2, got2, table, edge_out, edge_in, col_out, col_in,
    energy, moved, x_buf, h_buf, s_buf, coef_buf,
    z_send, z_recv, y_send, y_recv, x_send, x_recv, d_send, d_recv, a_send, a_recv, t_send, t_recv,
    e_send, e_recv, b_send, b_recv, halo_send, halo_recv, c_send, c_recv, local_sem,
):
    s = lax.axis_index("space")
    f = lax.axis_index("freq")
    core = s % 2
    x = (s // 2) % 4
    base = (s // 8) * 8
    y = f // 4
    zl = f % 4
    rb, cb = block_of(f)
    chans, rows, cols = spectrum.shape
    half = cols // 2
    groups = 16

    def at_freq(g):
        return {"space": s, "freq": g}

    def at_x(step):
        return {"space": base + ((x + step) % 4) * 2 + core, "freq": f}

    partner = {"space": s + 1 - 2 * core, "freq": f}
    above = {"space": jnp.maximum(s - 1, 0), "freq": f}
    below = {"space": jnp.minimum(s + 1, 15), "freq": f}
    has_up = jnp.logical_or(rb > 0, s > 0)
    has_down = jnp.logical_or(rb < 7, s < 15)
    up = {"space": jnp.where(rb > 0, s, jnp.maximum(s - 1, 0)), "freq": freq_of((rb + 7) % 8, cb)}
    down = {"space": jnp.where(rb < 7, s, jnp.minimum(s + 1, 15)), "freq": freq_of((rb + 1) % 8, cb)}
    beside = at_freq(freq_of(rb, 1 - cb))

    barrier = pltpu.get_barrier_semaphore()

    def greet(target):
        pl.semaphore_signal(barrier, inc=1, device_id=target, device_id_type=MESH)

    for k in range(1, groups):
        greet(at_freq((f + k) % 16))
    greet(at_x(1))
    greet(at_x(3))
    greet(partner)
    over_top = jnp.logical_and(rb == 0, s > 0)
    over_bottom = jnp.logical_and(rb == 7, s < 15)
    other_above = jnp.logical_and(core == 0, s > 0)
    other_below = jnp.logical_and(core == 1, s < 15)
    pl.when(over_top)(lambda: greet(up))
    pl.when(over_bottom)(lambda: greet(down))
    pl.when(other_above)(lambda: greet(above))
    pl.when(other_below)(lambda: greet(below))

    @pl.when(core == 0)
    def _():
        for k in range(9):
            own_w[k] = w_in[k].T

    @pl.when(core == 1)
    def _():
        for k in range(9):
            own_w[k] = w_out[:, k * 128 : (k + 1) * 128].T

    row_of = lax.broadcasted_iota(jnp.int32, (8, cols), 0)
    own_table[...] = jnp.where(
        row_of == 0, courant[0], jnp.where(row_of == 1, courant[1], jnp.where(row_of == 2, refract[0], refract[1]))
    )

    def turn(n):
        def some(c, carry):
            block = spectrum[pl.ds(c * 8, 8), pl.ds(n * 8, 8), :]
            field[pl.ds(n * 8 + 1, 8), pl.ds(pl.multiple_of(c * 8, 8), 8), :] = jnp.swapaxes(block, 0, 1)
            return carry

        lax.fori_loop(0, chans // 8, some, 0)

    turn(0)
    turn(3)
    known = (over_top, over_bottom, other_above, other_below)
    pl.semaphore_wait(barrier, 18 + sum(k.astype(jnp.int32) for k in known))

    def remote(src, dst, send, recv, target):
        return pltpu.make_async_remote_copy(
            src_ref=src, dst_ref=dst, send_sem=send, recv_sem=recv, device_id=target, device_id_type=MESH
        )

    def quarter(q):
        return pl.ds(pl.multiple_of(q * 32, 32), 32)

    own_quarter = weights.at[core, f, :, quarter(x), :]
    z_copies = []
    for k in range(1, 4):
        c = remote(
            own_w.at[:, quarter(x), :], own_quarter, z_send.at[k - 1], z_recv.at[k - 1], at_freq(y * 4 + (zl + k) % 4)
        )
        c.start()
        z_copies.append(c)
    to_above = remote(field.at[1], field.at[rows + 1], halo_send.at[0], halo_recv.at[1], above)
    to_below = remote(field.at[rows], field.at[0], halo_send.at[1], halo_recv.at[0], below)
    pl.when(s > 0)(to_above.start)
    pl.when(s < 15)(to_below.start)
    place = pltpu.make_async_copy(own_w.at[:, quarter(x), :], own_quarter, local_sem.at[0])
    place.start()
    table[f] = own_table[...]
    t_copies = []
    for k in range(1, groups):
        c = remote(own_table, table.at[f], t_send.at[k], t_recv.at[k], at_freq((f + k) % 16))
        c.start()
        t_copies.append(c)
    turn(1)
    turn(2)
    place.wait()

    def y_block(r, first=0, count=4, q=x):
        return weights.at[core, pl.ds(r * 4 + first, count), :, quarter(q), :]

    y_right, y_left = at_freq(((y + 1) % 4) * 4 + zl), at_freq(((y + 3) % 4) * 4 + zl)
    order = [y, (y + 3) % 4, (y + 1) % 4, (y + 2) % 4]
    xs = [x, (x + 3) % 4, (x + 1) % 4, (x + 2) % 4]
    y_copies, x_copies, d_copies = {}, {}, {}

    def go(where, key, copy):
        copy.start()
        where[key] = copy

    def spread(b):
        r = order[b]
        block = y_block(r)
        go(x_copies, (b, 0), remote(block, block, x_send.at[b, 0], x_recv.at[b, 0], at_x(1)))
        go(x_copies, (b, 1), remote(block, block, x_send.at[b, 1], x_recv.at[b, 1], at_x(3)))
        share(b, 0)

    def share(b, k):
        block = y_block(order[b], q=xs[k])
        go(d_copies, (b, k), remote(block, block, d_send.at[b, k], d_recv.at[b, k], partner))

    def weights_1():
        for c in z_copies:
            c.wait_recv()
        own = y_block(y)
        go(y_copies, 0, remote(own, own, y_send.at[0], y_recv.at[0], y_right))
        go(y_copies, 1, remote(own, own, y_send.at[1], y_recv.at[1], y_left))
        spread(0)

    def weights_2():
        y_copies[0].wait_recv()
        part = y_block(order[1], 0, 2)
        go(y_copies, 2, remote(part, part, y_send.at[2], y_recv.at[2], y_right))
        spread(1)

    def weights_3():
        y_copies[1].wait_recv()
        part = y_block(order[2], 2, 2)
        go(y_copies, 3, remote(part, part, y_send.at[3], y_recv.at[3], y_left))
        spread(2)

    def weights_4():
        y_copies[2].wait_recv()
        y_copies[3].wait_recv()
        spread(3)

    def weights_5(b):
        x_copies[b, 0].wait_recv()
        part = y_block(order[b], 0, 2, xs[1])
        go(x_copies, (b, 2), remote(part, part, x_send.at[b, 2], x_recv.at[b, 2], at_x(1)))
        share(b, 1)
        x_copies[b, 1].wait_recv()
        part = y_block(order[b], 2, 2, xs[2])
        go(x_copies, (b, 3), remote(part, part, x_send.at[b, 3], x_recv.at[b, 3], at_x(3)))
        share(b, 2)

    def weights_6(b):
        x_copies[b, 2].wait_recv()
        x_copies[b, 3].wait_recv()
        share(b, 3)

    coef = coefficients(own_table[...], cos_ref[...], sin_ref[...])
    for i, c in enumerate(coef):
        coef_buf[i] = c

    @pl.when(s > 0)
    def _():
        to_below.wait_recv()

    @pl.when(s == 0)
    def _():
        field[0] = jnp.zeros((chans, cols), jnp.float32)

    @pl.when(s < 15)
    def _():
        to_above.wait_recv()

    @pl.when(s == 15)
    def _():
        field[rows + 1] = jnp.zeros((chans, cols), jnp.float32)

    def first_rows(n):
        def one(r, carry):
            row = n * 4 + r
            value = transport_row(
                field[row], field[row + 1], field[row + 2], 0.0, 0.0, [coef_buf[i] for i in range(7)],
                dx[pl.ds(row, 1), :], dy[pl.ds(row, 1), :], land[pl.ds(row, 1), :].astype(jnp.float32),
            )
            code = encode(value, TOP_T1)
            codes1[n * 2, r] = code[:, :half]
            codes1[n * 2 + 1, r] = code[:, half:]
            return carry

        lax.fori_loop(0, 4, one, 0)

    def first_copy(k, c):
        n = (rb + k) % 8
        return remote(codes1.at[n * 2 + c], got1.at[f], a_send.at[k, c], a_recv.at[k, cb], at_freq(freq_of(n, c)))

    def first_and_send(k, carry):
        first_rows((rb + k) % 8)
        first_copy(k, 0).start()
        first_copy(k, 1).start()
        return carry

    lax.fori_loop(1, 8, first_and_send, 0)
    first_rows(rb)
    first_copy(0, 1 - cb).start()
    mine = pltpu.make_async_copy(codes1.at[rb * 2 + cb], got1.at[f], local_sem.at[0])
    mine.start()
    weights_1()
    weights_2()
    weights_3()
    weights_4()
    mine.wait()
    for b in range(4):
        weights_5(b)

    def first_arrival(k, c):
        g = freq_of((rb + 8 - k) % 8, c)
        return remote(codes1.at[0], got1.at[g], a_send.at[k, 0], a_recv.at[k, c], at_freq(g))

    def await_rows(k, carry):
        first_arrival(k, 0).wait_recv()
        first_arrival(k, 1).wait_recv()
        return carry

    lax.fori_loop(1, 8, await_rows, 0)
    first_arrival(0, 1 - cb).wait_recv()
    for b in range(4):
        weights_6(b)
    for c in d_copies.values():
        c.wait_recv()

    def network():
        def first_layer(i, carry):
            lhs = jnp.concatenate(
                [
                    jnp.concatenate([weights[0, i * 4 + q, k] for k in range(9)], axis=1)
                    for q in range(4)
                ],
                axis=0,
            )
            pre = jnp.dot(lhs, x_buf[...], preferred_element_type=jnp.float32)
            h_buf[pl.ds(pl.multiple_of(i * 512, 512), 512), :] = gelu(pre).astype(jnp.bfloat16)
            return carry

        lax.fori_loop(0, 4, first_layer, 0)

        def second_layer(i, carry):
            lhs = jnp.concatenate(
                [
                    jnp.concatenate([weights[1, g, i * 3 + k] for g in range(16)], axis=1)
                    for k in range(3)
                ],
                axis=0,
            )
            s_buf[pl.ds(pl.multiple_of(i * 384, 384), 384), :] = jnp.dot(
                lhs, h_buf[...], preferred_element_type=jnp.float32
            )
            return carry

        lax.fori_loop(0, 3, second_layer, 0)

    def scale_into_x(total):
        mean = jnp.sum(total, axis=0, keepdims=True) * (1.0 / 1152.0) + epsilon
        inverse = 1.0 / mean

        def pair(p, carry):
            both = jnp.concatenate([moved[p * 2], moved[p * 2 + 1]], axis=0) * inverse
            x_buf[pl.ds(pl.multiple_of(p * 144, 144), 144), :] = both.astype(jnp.bfloat16)
            return carry

        lax.fori_loop(0, 8, pair, 0)

    def growth(g):
        return jnp.exp(step_scale * jnp.tanh(s_buf[pl.ds(pl.multiple_of(g * 72, 8), 72), :]))

    zeros = jnp.zeros((chans, cols), jnp.float32)
    thin = zeros[:, :half]
    lane = lax.broadcasted_iota(jnp.int32, (chans, half), 1)

    edge_copies = [
        remote(edge_out.at[0], edge_in.at[1], e_send.at[0], e_recv.at[1], up),
        remote(edge_out.at[1], edge_in.at[0], e_send.at[1], e_recv.at[0], down),
    ]
    for first, last in ((0, 3), (1, 2)):

        def load(g, total):
            value = decode(jnp.concatenate([got1[g, first], got1[g, last]], axis=1), TOP_T1)
            moved[g] = value
            return total + value

        scale_into_x(lax.fori_loop(0, groups, load, zeros))
        network()

        def update(g, carry):
            value = moved[g] * growth(g)
            energy[g, first + 1] = value[:, :half]
            energy[g, last + 1] = value[:, half:]
            if first == 0:
                code = encode(value, TOP_E1)
                edge_out[0, g] = code[:, :half]
                edge_out[1, g] = code[:, half:]
            return carry

        lax.fori_loop(0, groups, update, 0)
        if first == 0:
            pl.when(has_up)(edge_copies[0].start)
            pl.when(has_down)(edge_copies[1].start)

    edge_lane = (half - 1) * (1 - cb)

    def pack(g, block):
        for r in range(4):
            at = g * 4 + r
            turned = pltpu.roll(energy[g, r + 1], (at - edge_lane + half) % half, 1)
            block = jnp.where(lane == at, turned, block)
        return block

    col_out[...] = lax.fori_loop(0, groups, pack, thin)
    col_copy = remote(col_out, col_in, c_send.at[0], c_recv.at[0], beside)
    col_copy.start()
    for k in range(1, groups):
        t_copies[k - 1].wait_recv()
    west_side = cb.astype(jnp.float32)
    land_lane = (half - 1) * (1 - cb)

    def my_half(line):
        return jnp.where(cb == 0, line[:, :half], line[:, half:])

    col_copy.wait_recv()

    def fill(present, copy, slot, row):
        @pl.when(present)
        def _():
            copy.wait_recv()

            def some(g, carry):
                energy[g, row] = decode(edge_in[slot, g], TOP_E1)
                return carry

            lax.fori_loop(0, groups, some, 0)

        @pl.when(jnp.logical_not(present))
        def _():
            def some(g, carry):
                energy[g, row] = thin
                return carry

            lax.fori_loop(0, groups, some, 0)

    for n, pair in enumerate(((1, 2), (0, 3))):
        if n == 1:
            fill(has_up, edge_copies[1], 0, 0)
            fill(has_down, edge_copies[0], 1, 5)

        def second(g, total):
            coef = coefficients(table[g][:, :half], cos_ref[:, :half], sin_ref[:, :half])
            done = []
            for r in pair:
                row = pl.ds(rb * 4 + r, 1)
                side = pltpu.roll(col_in[...], (land_lane - (g * 4 + r) + half) % half, 1)
                done.append(
                    transport_row(
                        energy[g, r], energy[g, r + 1], energy[g, r + 2], side * west_side, side * (1.0 - west_side),
                        coef, my_half(dx[row, :]), my_half(dy[row, :]), my_half(land[row, :]).astype(jnp.float32),
                    )
                )
            value = jnp.concatenate(done, axis=1)
            moved[g] = value
            return total + value

        scale_into_x(lax.fori_loop(0, groups, second, zeros))
        network()

        def finish(k):
            g = (f + k) % 16
            code = encode(moved[g] * growth(g), TOP_E2)
            codes2[g, n * 2] = code[:, :half]
            codes2[g, n * 2 + 1] = code[:, half:]

        def finish_and_send(k, carry):
            finish(k)
            g = (f + k) % 16
            two = pl.ds(n * 2, 2)
            remote(codes2.at[g, two], got2.at[rb * 2 + cb, two], b_send.at[n, k], b_recv.at[n, k], at_freq(g)).start()
            return carry

        lax.fori_loop(1, groups, finish_and_send, 0)
        finish(0)

    own_back = pltpu.make_async_copy(codes2.at[f], got2.at[rb * 2 + cb], local_sem.at[0])
    own_back.start()

    def await_back(k, carry):
        g = (f + 16 - k) % 16
        b, c = block_of(g)
        for n in range(2):
            two = pl.ds(n * 2, 2)
            remote(codes2.at[0, two], got2.at[b * 2 + c, two], b_send.at[n, k], b_recv.at[n, k], at_freq(g)).wait_recv()
        return carry

    lax.fori_loop(1, groups, await_back, 0)
    own_back.wait()

    def put(j, carry):
        out[j] = got2[j]
        return carry

    lax.fori_loop(0, groups, put, 0)

    for c in z_copies + t_copies + list(y_copies.values()) + list(x_copies.values()) + list(d_copies.values()):
        c.wait_send()

    def sent(k, carry):
        for n in range(2):
            two = pl.ds(n * 2, 2)
            remote(codes2.at[0, two], got2.at[0, two], b_send.at[n, k], b_recv.at[n, k], partner).wait_send()
        return carry

    lax.fori_loop(1, groups, sent, 0)

    def sent_first(k, carry):
        first_copy(k, 0).wait_send()
        first_copy(k, 1).wait_send()
        return carry

    lax.fori_loop(1, 8, sent_first, 0)
    first_copy(0, 1 - cb).wait_send()
    col_copy.wait_send()
    pl.when(s > 0)(to_above.wait_send)
    pl.when(s < 15)(to_below.wait_send)
    pl.when(has_up)(edge_copies[0].wait_send)
    pl.when(has_down)(edge_copies[1].wait_send)


def turn_back(codes, out):
    chans = out.shape[0]
    half = codes.shape[-1]
    slot = (2, 0, 1, 3)

    def some(c, carry):
        part = pl.ds(pl.multiple_of(c * 8, 8), 8)
        for side in range(2):
            lines = [decode(codes[n, side, slot[r], part, :], TOP_E2)[None] for n in range(2) for r in range(4)]
            out[part, :, side * half : (side + 1) * half] = jnp.swapaxes(jnp.concatenate(lines, axis=0), 0, 1)
        return carry

    lax.fori_loop(0, chans // 8, some, 0)


def body(spectrum, land_sea, courant, refract, depth_dx, depth_dy, w_in, w_out):
    freqs, dirs, rows, cols = spectrum.shape
    chans = freqs * dirs
    half = cols // 2
    angles = (np.arange(DIRS, dtype=np.float32) + np.float32(0.5)) * np.float32(2.0 * math.pi / DIRS)
    cos_table = np.ascontiguousarray(np.broadcast_to(np.tile(np.cos(angles), freqs)[:, None], (chans, cols)))
    sin_table = np.ascontiguousarray(np.broadcast_to(np.tile(np.sin(angles), freqs)[:, None], (chans, cols)))
    vmem = pl.BlockSpec(memory_space=pltpu.VMEM)
    smem = pl.BlockSpec(memory_space=pltpu.SMEM)
    dma = pltpu.SemaphoreType.DMA
    i16, f32, b16 = jnp.int16, jnp.float32, jnp.bfloat16
    back = pl.pallas_call(
        kernel,
        out_shape=jax.ShapeDtypeStruct((16, 4, chans, half), i16),
        in_specs=[vmem] * 4 + [smem] * 2 + [vmem] * 4,
        out_specs=vmem,
        scratch_shapes=[
            pltpu.VMEM((rows + 2, chans, cols), f32),
            pltpu.VMEM((8, cols), f32),
            pltpu.VMEM((9, 128, 128), b16),
            pltpu.VMEM((2, 16, 9, 128, 128), b16),
            pltpu.VMEM((16, 4, chans, half), i16),
            pltpu.VMEM((16, 4, chans, half), i16),
            pltpu.VMEM((16, 4, chans, half), i16),
            pltpu.VMEM((16, 4, chans, half), i16),
            pltpu.VMEM((16, 8, cols), f32),
            pltpu.VMEM((2, 16, chans, half), i16),
            pltpu.VMEM((2, 16, chans, half), i16),
            pltpu.VMEM((chans, half), f32),
            pltpu.VMEM((chans, half), f32),
            pltpu.VMEM((16, 6, chans, half), f32),
            pltpu.VMEM((16, chans, cols), f32),
            pltpu.VMEM((16 * chans, cols), b16),
            pltpu.VMEM((2048, cols), b16),
            pltpu.VMEM((16 * chans, cols), f32),
            pltpu.VMEM((7, chans, cols), f32),
            dma((3,)), dma((3,)), dma((4,)), dma((4,)), dma((4, 4)), dma((4, 4)), dma((4, 4)), dma((4, 4)),
            dma((8, 2)), dma((8, 2)), dma((16,)), dma((16,)), dma((2,)), dma((2,)), dma((2, 16)), dma((2, 16)),
            dma((2,)), dma((2,)), dma((1,)), dma((1,)), dma((1,)),
        ],
        compiler_params=pltpu.CompilerParams(
            collective_id=0, has_side_effects=True, vmem_limit_bytes=60 * 1024 * 1024
        ),
    )(
        spectrum.reshape(chans, rows, cols), depth_dx, depth_dy, land_sea, courant, refract, cos_table, sin_table,
        w_in.reshape(9, 128, 128), w_out,
    )
    result = pl.pallas_call(
        turn_back,
        grid=(4,),
        out_shape=jax.ShapeDtypeStruct((chans, rows, cols), f32),
        in_specs=[pl.BlockSpec((2, 2, 4, chans, half), lambda i: (i, 0, 0, 0, 0))],
        out_specs=pl.BlockSpec((chans, 8, cols), lambda i: (0, i, 0)),
    )(back.reshape(8, 2, 4, chans, half))
    return result.reshape(freqs, dirs, rows, cols)


def solution(mesh):
    placed = (
        P("freq", None, "space", None),
        P("space", None),
        P("freq"),
        P("freq"),
        P("space", None),
        P("space", None),
        P(None, "freq"),
        P("freq", None),
    )
    return jax.shard_map(
        body, mesh=mesh, in_specs=placed, out_specs=P("freq", None, "space", None), check_vma=False
    )
```

```python
import math

import jax
import jax.numpy as jnp
import numpy as np
from jax import lax
from jax.experimental import pallas as pl
from jax.experimental.pallas import tpu as pltpu
from jax.sharding import PartitionSpec as P

DIRS = 36
MESH = pl.DeviceIdType.MESH

step_scale = 0.5
epsilon = 1e-06

TOP_T1 = 2.45
TOP_E1 = 4.06
TOP_E2 = 8.2
LEVELS = 65535.0
HALF = 32768.0


def encode(value, top):
    level = jnp.minimum(value * (LEVELS / top) + 0.5, LEVELS)
    return (level.astype(jnp.int32) - 32768).astype(jnp.int16)


def decode(code, top):
    return (code.astype(jnp.int32).astype(jnp.float32) + HALF) * (top / LEVELS)


def freq_of(rb, cb):
    high = rb // 4
    yy = rb % 4
    return (yy + high * (3 - 2 * yy)) * 4 + high * 2 + cb


def block_of(f):
    y = f // 4
    zl = f % 4
    high = zl // 2
    return high * 4 + y + high * (3 - 2 * y), zl % 2


def coefficients(table, cosine, sine):
    first = lax.broadcasted_iota(jnp.int32, cosine.shape, 0) < DIRS
    courant = jnp.where(first, table[0:1], table[1:2])
    refract = jnp.where(first, table[2:3], table[3:4])
    speed_x = courant * cosine
    speed_y = courant * sine
    pos_x = jnp.maximum(speed_x, 0.0)
    pos_y = jnp.maximum(speed_y, 0.0)
    keep = 1.0 - jnp.abs(speed_x) - jnp.abs(speed_y)
    return keep, pos_x, pos_x - speed_x, pos_y, pos_y - speed_y, refract * sine, refract * cosine


def transport_row(before, center, after, west_edge, east_edge, coef, dx, dy, sea):
    keep, pos_x, neg_x, pos_y, neg_y, turn_x, turn_y = coef
    rows, cols = center.shape
    lane = lax.broadcasted_iota(jnp.int32, center.shape, 1)
    west = jnp.where(lane == 0, west_edge, pltpu.roll(center, 1, 1))
    east = jnp.where(lane == cols - 1, east_edge, pltpu.roll(center, cols - 1, 1))
    shifted = center * keep + pos_x * before + neg_x * after + pos_y * west + neg_y * east
    turning = (turn_x * dx - turn_y * dy) * shifted
    moved_up = jnp.maximum(turning, 0.0)
    moved_down = jnp.maximum(-turning, 0.0)
    d = lax.broadcasted_iota(jnp.int32, center.shape, 0)
    lower = jnp.where((d == 0) | (d == DIRS), pltpu.roll(moved_up, DIRS + 1, 0), pltpu.roll(moved_up, 1, 0))
    upper = jnp.where(
        (d == DIRS - 1) | (d == rows - 1),
        pltpu.roll(moved_down, DIRS - 1, 0),
        pltpu.roll(moved_down, rows - 1, 0),
    )
    return (shifted - jnp.abs(turning) + lower + upper) * sea


def gelu(x):
    return 0.5 * x * (1.0 + jnp.tanh(math.sqrt(2.0 / math.pi) * (x + 0.044715 * x * x * x)))


def kernel(
    spectrum_in, dx_in, dy_in, land_in, courant, refract, cos_in, sin_in, w_in_in, w_out_in, out,
    spectrum, dx, dy, land, cos_ref, sin_ref, w_in, w_out,
    field, own_table, own_w, weights, codes1, got1, codes2, got2, table, edge_out, edge_in, col_out, col_in,
    energy, moved, x_buf, h_buf, s_buf, coef_buf,
    z_send, z_recv, y_send, y_recv, x_send, x_recv, d_send, d_recv, a_send, a_recv, t_send, t_recv,
    e_send, e_recv, b_send, b_recv, halo_send, halo_recv, c_send, c_recv, l_send, l_recv, m_send, m_recv,
    local_sem, load_sem, store_sem,
):
    s = lax.axis_index("space")
    f = lax.axis_index("freq")
    core = s % 2
    x = (s // 2) % 4
    base = (s // 8) * 8
    y = f // 4
    zl = f % 4
    rb, cb = block_of(f)
    chans, rows, cols = spectrum.shape
    half = cols // 2
    groups = 16

    def at_freq(g):
        return {"space": s, "freq": g}

    def at_x(step):
        return {"space": base + ((x + step) % 4) * 2 + core, "freq": f}

    partner = {"space": s + 1 - 2 * core, "freq": f}
    above = {"space": jnp.maximum(s - 1, 0), "freq": f}
    below = {"space": jnp.minimum(s + 1, 15), "freq": f}
    has_up = jnp.logical_or(rb > 0, s > 0)
    has_down = jnp.logical_or(rb < 7, s < 15)
    up = {"space": jnp.where(rb > 0, s, jnp.maximum(s - 1, 0)), "freq": freq_of((rb + 7) % 8, cb)}
    down = {"space": jnp.where(rb < 7, s, jnp.minimum(s + 1, 15)), "freq": freq_of((rb + 1) % 8, cb)}
    beside = at_freq(freq_of(rb, 1 - cb))

    barrier = pltpu.get_barrier_semaphore()

    def greet(target):
        pl.semaphore_signal(barrier, inc=1, device_id=target, device_id_type=MESH)

    for k in range(1, groups):
        greet(at_freq((f + k) % 16))
    greet(at_x(1))
    greet(at_x(3))
    greet(partner)
    over_top = jnp.logical_and(rb == 0, s > 0)
    over_bottom = jnp.logical_and(rb == 7, s < 15)
    other_above = jnp.logical_and(core == 0, s > 0)
    other_below = jnp.logical_and(core == 1, s < 15)
    pl.when(over_top)(lambda: greet(up))
    pl.when(over_bottom)(lambda: greet(down))
    pl.when(other_above)(lambda: greet(above))
    pl.when(other_below)(lambda: greet(below))

    loads = [
        pltpu.make_async_copy(src, dst, load_sem.at[i])
        for i, (src, dst) in enumerate(
            (
                (w_in_in, w_in), (w_out_in, w_out), (spectrum_in, spectrum), (cos_in, cos_ref), (sin_in, sin_ref),
                (dx_in, dx), (dy_in, dy), (land_in, land),
            )
        )
    ]
    for c in loads:
        c.start()
    loads[0].wait()
    loads[1].wait()

    @pl.when(core == 0)
    def _():
        for k in range(9):
            own_w[k] = w_in[k].T

    @pl.when(core == 1)
    def _():
        for k in range(9):
            own_w[k] = w_out[:, k * 128 : (k + 1) * 128].T

    row_of = lax.broadcasted_iota(jnp.int32, (8, cols), 0)
    own_table[...] = jnp.where(
        row_of == 0, courant[0], jnp.where(row_of == 1, courant[1], jnp.where(row_of == 2, refract[0], refract[1]))
    )

    def turn(n):
        def some(c, carry):
            block = spectrum[pl.ds(c * 8, 8), pl.ds(n * 8, 8), :]
            field[pl.ds(n * 8 + 1, 8), pl.ds(pl.multiple_of(c * 8, 8), 8), :] = jnp.swapaxes(block, 0, 1)
            return carry

        lax.fori_loop(0, chans // 8, some, 0)

    loads[2].wait()
    turn(0)
    turn(3)
    known = (over_top, over_bottom, other_above, other_below)
    pl.semaphore_wait(barrier, 18 + sum(k.astype(jnp.int32) for k in known))

    def remote(src, dst, send, recv, target):
        return pltpu.make_async_remote_copy(
            src_ref=src, dst_ref=dst, send_sem=send, recv_sem=recv, device_id=target, device_id_type=MESH
        )

    def quarter(q):
        return pl.ds(pl.multiple_of(q * 32, 32), 32)

    own_quarter = weights.at[core, f, :, quarter(x), :]
    z_copies = []
    for k in range(1, 4):
        c = remote(
            own_w.at[:, quarter(x), :], own_quarter, z_send.at[k - 1], z_recv.at[k - 1], at_freq(y * 4 + (zl + k) % 4)
        )
        c.start()
        z_copies.append(c)
    to_above = remote(field.at[1], field.at[rows + 1], halo_send.at[0], halo_recv.at[1], above)
    to_below = remote(field.at[rows], field.at[0], halo_send.at[1], halo_recv.at[0], below)
    pl.when(s > 0)(to_above.start)
    pl.when(s < 15)(to_below.start)
    place = pltpu.make_async_copy(own_w.at[:, quarter(x), :], own_quarter, local_sem.at[0])
    place.start()
    table[f] = own_table[...]
    t_copies = []
    for k in range(1, groups):
        c = remote(own_table, table.at[f], t_send.at[k], t_recv.at[k], at_freq((f + k) % 16))
        c.start()
        t_copies.append(c)
    turn(1)
    turn(2)
    for c in loads[3:]:
        c.wait()
    place.wait()

    y_right, y_left = at_freq(((y + 1) % 4) * 4 + zl), at_freq(((y + 3) % 4) * 4 + zl)
    order = [y, (y + 3) % 4, (y + 1) % 4, (y + 2) % 4]
    xs = [x, (x + 3) % 4, (x + 1) % 4, (x + 2) % 4]
    whole, front, rear = (0, 9), (0, 5), (5, 4)
    copies = {}

    def by_quarter(b, q, ks=whole, count=None):
        count = (4 if b == 0 else 3) if count is None else count
        return weights.at[core, pl.ds(order[b] * 4, count), pl.ds(*ks), quarter(q), :]

    def by_piece(b, ks=whole):
        return weights.at[core, order[b] * 4 + 3, pl.ds(*ks)]

    def go(key, block, send, recv, target):
        c = remote(block, block, send, recv, target)
        c.start()
        copies[key] = c

    def got(*key):
        copies[key].wait_recv()

    def spread(b):
        block = by_quarter(b, x)
        go(("x", b, 0), block, x_send.at[b, 0], x_recv.at[b, 0], at_x(1))
        go(("x", b, 1), block, x_send.at[b, 1], x_recv.at[b, 1], at_x(3))
        share(b, 0)

    def share(b, k):
        go(("d", b, k), by_quarter(b, xs[k]), d_send.at[b, k], d_recv.at[b, k], partner)

    def share_piece(b):
        go(("m", b), by_piece(b), m_send.at[b], m_recv.at[b], partner)

    def weights_1():
        for c in z_copies:
            c.wait_recv()
        own = by_quarter(0, x, count=3)
        go(("y", 0), own, y_send.at[0], y_recv.at[0], y_right)
        go(("y", 1), own, y_send.at[1], y_recv.at[1], y_left)
        spread(0)

    def weights_2():
        got("y", 0)
        go(("y", 2), by_quarter(1, x, front), y_send.at[2], y_recv.at[2], y_right)
        spread(1)

    def weights_3():
        got("y", 1)
        go(("y", 3), by_quarter(2, x, rear), y_send.at[3], y_recv.at[3], y_left)
        spread(2)

    def weights_4():
        got("y", 2)
        got("y", 3)
        spread(3)

    def weights_5(b):
        got("x", b, 0)
        go(("x", b, 2), by_quarter(b, xs[1], front), x_send.at[b, 2], x_recv.at[b, 2], at_x(1))
        share(b, 1)
        got("x", b, 1)
        go(("x", b, 3), by_quarter(b, xs[2], rear), x_send.at[b, 3], x_recv.at[b, 3], at_x(3))
        share(b, 2)

    def weights_6(b):
        got("x", b, 2)
        got("x", b, 3)
        share(b, 3)

    def pieces_1():
        go(("l", 0), by_piece(0), l_send.at[0], l_recv.at[0], y_right)
        go(("l", 1), by_piece(0), l_send.at[1], l_recv.at[1], y_left)

    def pieces_2():
        got("l", 0)
        go(("l", 2), by_piece(1, front), l_send.at[2], l_recv.at[2], y_right)
        share_piece(1)
        got("l", 1)
        go(("l", 3), by_piece(2, rear), l_send.at[3], l_recv.at[3], y_left)
        share_piece(2)

    def pieces_3():
        got("l", 2)
        got("l", 3)
        share_piece(3)

    coef = coefficients(own_table[...], cos_ref[...], sin_ref[...])
    for i, c in enumerate(coef):
        coef_buf[i] = c

    @pl.when(s > 0)
    def _():
        to_below.wait_recv()

    @pl.when(s == 0)
    def _():
        field[0] = jnp.zeros((chans, cols), jnp.float32)

    @pl.when(s < 15)
    def _():
        to_above.wait_recv()

    @pl.when(s == 15)
    def _():
        field[rows + 1] = jnp.zeros((chans, cols), jnp.float32)

    def first_rows(n):
        def one(r, carry):
            row = n * 4 + r
            value = transport_row(
                field[row], field[row + 1], field[row + 2], 0.0, 0.0, [coef_buf[i] for i in range(7)],
                dx[pl.ds(row, 1), :], dy[pl.ds(row, 1), :], land[pl.ds(row, 1), :].astype(jnp.float32),
            )
            code = encode(value, TOP_T1)
            codes1[n * 2, r] = code[:, :half]
            codes1[n * 2 + 1, r] = code[:, half:]
            return carry

        lax.fori_loop(0, 4, one, 0)

    def first_copy(i):
        ky, kz = i // 4, i % 4
        g = ((y + ky) % 4) * 4 + (zl + kz) % 4
        n, c = block_of(g)
        return remote(codes1.at[n * 2 + c], got1.at[f], a_send.at[i], a_recv.at[i], at_freq(g))

    def first_send(i, carry):
        first_copy(i).start()
        return carry

    def first_arrival(i, carry):
        g = ((y + 4 - i // 4) % 4) * 4 + (zl + 4 - i % 4) % 4
        remote(codes1.at[0], got1.at[g], a_send.at[i], a_recv.at[i], at_freq(g)).wait_recv()
        return carry

    def all_rows(n, carry):
        first_rows(n)
        return carry

    lax.fori_loop(0, 8, all_rows, 0)
    mine = pltpu.make_async_copy(codes1.at[rb * 2 + cb], got1.at[f], local_sem.at[0])
    mine.start()
    weights_1()
    lax.fori_loop(1, 4, first_send, 0)
    weights_2()
    weights_5(0)
    weights_3()
    lax.fori_loop(4, 16, first_send, 0)
    mine.wait()
    weights_4()
    weights_6(0)
    pieces_1()
    weights_5(1)
    weights_5(2)
    pieces_2()

    def rows_of(hidden, blocks, size):
        for n, at in enumerate(blocks):
            yield pl.ds(pl.multiple_of(at, size), size), hidden[n * size : (n + 1) * size]

    def first_quarter(q, p):
        pieces = [b * 4 + n for b in range(4) for n in range(3)]
        lhs = jnp.concatenate(
            [jnp.concatenate([weights[0, g, k, quarter(q), :] for k in range(9)], axis=1) for g in pieces], axis=0
        )
        hidden = gelu(jnp.dot(lhs, x_buf[p], preferred_element_type=jnp.float32)).astype(jnp.bfloat16)
        for where, part in rows_of(hidden, [g * 128 + q * 32 for g in pieces], 32):
            h_buf[p, where, :] = part

    def first_rest(p):
        pieces = [b * 4 + 3 for b in range(4)]
        lhs = jnp.concatenate(
            [jnp.concatenate([weights[0, g, k] for k in range(9)], axis=1) for g in pieces], axis=0
        )
        hidden = gelu(jnp.dot(lhs, x_buf[p], preferred_element_type=jnp.float32)).astype(jnp.bfloat16)
        for where, part in rows_of(hidden, [g * 128 for g in pieces], 128):
            h_buf[p, where, :] = part

    def second_layer(p):
        def some(i, carry):
            lhs = jnp.concatenate(
                [
                    jnp.concatenate([weights[1, g, i * 3 + k] for g in range(16)], axis=1)
                    for k in range(3)
                ],
                axis=0,
            )
            s_buf[pl.ds(pl.multiple_of(i * 384, 384), 384), :] = jnp.dot(
                lhs, h_buf[p], preferred_element_type=jnp.float32
            )
            return carry

        lax.fori_loop(0, 3, some, 0)

    def scale_into_x(total, p):
        mean = jnp.sum(total, axis=0, keepdims=True) * (1.0 / 1152.0) + epsilon
        inverse = 1.0 / mean

        def pair(n, carry):
            both = jnp.concatenate([moved[n * 2], moved[n * 2 + 1]], axis=0) * inverse
            x_buf[p, pl.ds(pl.multiple_of(n * 144, 144), 144), :] = both.astype(jnp.bfloat16)
            return carry

        lax.fori_loop(0, 8, pair, 0)

    def growth(g):
        return jnp.exp(step_scale * jnp.tanh(s_buf[pl.ds(pl.multiple_of(g * 72, 8), 72), :]))

    zeros = jnp.zeros((chans, cols), jnp.float32)
    thin = zeros[:, :half]
    lane = lax.broadcasted_iota(jnp.int32, (chans, half), 1)

    edge_copies = [
        remote(edge_out.at[0], edge_in.at[1], e_send.at[0], e_recv.at[1], up),
        remote(edge_out.at[1], edge_in.at[0], e_send.at[1], e_recv.at[0], down),
    ]
    lax.fori_loop(1, 16, first_arrival, 0)
    pairs = ((0, 3), (1, 2))

    def both_of(g, pair):
        return decode(jnp.concatenate([got1[g, pair[0]], got1[g, pair[1]]], axis=1), TOP_T1)

    for p in range(2):

        def load(g, total):
            value = both_of(g, pairs[p])
            moved[g] = value
            return total + value

        scale_into_x(lax.fori_loop(0, groups, load, zeros), p)

    def first_layer_of(i):
        for b in range(4):
            got("d", b, i)

        def one(p, carry):
            first_quarter(xs[i], p)
            return carry

        lax.fori_loop(0, 2, one, 0)

    first_layer_of(0)
    weights_5(3)
    pieces_3()
    first_layer_of(1)
    weights_6(1)
    first_layer_of(2)
    weights_6(2)
    weights_6(3)
    first_layer_of(3)
    for b in range(1, 4):
        got("m", b)

    def last_one(p, carry):
        first_rest(p)
        return carry

    lax.fori_loop(0, 2, last_one, 0)
    for p, (first, last) in enumerate(pairs):
        second_layer(p)

        def update(g, carry):
            value = both_of(g, pairs[p]) * growth(g)
            energy[g, first + 1] = value[:, :half]
            energy[g, last + 1] = value[:, half:]
            if first == 0:
                code = encode(value, TOP_E1)
                edge_out[0, g] = code[:, :half]
                edge_out[1, g] = code[:, half:]
            return carry

        lax.fori_loop(0, groups, update, 0)
        if first == 0:
            pl.when(has_up)(edge_copies[0].start)
            pl.when(has_down)(edge_copies[1].start)

    edge_lane = (half - 1) * (1 - cb)

    def pack(g, block):
        for r in range(4):
            at = g * 4 + r
            turned = pltpu.roll(energy[g, r + 1], (at - edge_lane + half) % half, 1)
            block = jnp.where(lane == at, turned, block)
        return block

    col_out[...] = lax.fori_loop(0, groups, pack, thin, unroll=4)
    col_copy = remote(col_out, col_in, c_send.at[0], c_recv.at[0], beside)
    col_copy.start()
    for k in range(1, groups):
        t_copies[k - 1].wait_recv()
    west_side = cb.astype(jnp.float32)
    land_lane = (half - 1) * (1 - cb)

    def my_half(line):
        return jnp.where(cb == 0, line[:, :half], line[:, half:])

    col_copy.wait_recv()

    def fill(present, copy, slot, row):
        @pl.when(present)
        def _():
            copy.wait_recv()

            def some(g, carry):
                energy[g, row] = decode(edge_in[slot, g], TOP_E1)
                return carry

            lax.fori_loop(0, groups, some, 0)

        @pl.when(jnp.logical_not(present))
        def _():
            def some(g, carry):
                energy[g, row] = thin
                return carry

            lax.fori_loop(0, groups, some, 0)

    for n, pair in enumerate(((1, 2), (0, 3))):
        if n == 1:
            fill(has_up, edge_copies[1], 0, 0)
            fill(has_down, edge_copies[0], 1, 5)

        def second(g, total):
            coef = coefficients(table[g][:, :half], cos_ref[:, :half], sin_ref[:, :half])
            done = []
            for r in pair:
                row = pl.ds(rb * 4 + r, 1)
                side = pltpu.roll(col_in[...], (land_lane - (g * 4 + r) + half) % half, 1)
                done.append(
                    transport_row(
                        energy[g, r], energy[g, r + 1], energy[g, r + 2], side * west_side, side * (1.0 - west_side),
                        coef, my_half(dx[row, :]), my_half(dy[row, :]), my_half(land[row, :]).astype(jnp.float32),
                    )
                )
            value = jnp.concatenate(done, axis=1)
            moved[g] = value
            return total + value

        scale_into_x(lax.fori_loop(0, groups, second, zeros), n)

        def quarters(q, carry):
            first_quarter(q, n)
            return carry

        lax.fori_loop(0, 4, quarters, 0)
        first_rest(n)
        second_layer(n)

        def finish(k):
            g = (f + k) % 16
            code = encode(moved[g] * growth(g), TOP_E2)
            codes2[g, n * 2] = code[:, :half]
            codes2[g, n * 2 + 1] = code[:, half:]

        def finish_and_send(k, carry):
            finish(k)
            g = (f + k) % 16
            two = pl.ds(n * 2, 2)
            remote(codes2.at[g, two], got2.at[rb * 2 + cb, two], b_send.at[n, k], b_recv.at[n, k], at_freq(g)).start()
            return carry

        lax.fori_loop(1, groups, finish_and_send, 0)
        finish(0)

    own_back = pltpu.make_async_copy(codes2.at[f], got2.at[rb * 2 + cb], local_sem.at[0])
    own_back.start()

    def await_back(k, carry):
        g = (f + 16 - k) % 16
        b, c = block_of(g)
        for n in range(2):
            two = pl.ds(n * 2, 2)
            remote(codes2.at[0, two], got2.at[b * 2 + c, two], b_send.at[n, k], b_recv.at[n, k], at_freq(g)).wait_recv()
        put(b * 2 + c).start()
        return carry

    def put(n):
        return pltpu.make_async_copy(got2.at[n], out.at[n], store_sem.at[n])

    own_back.wait()
    put(rb * 2 + cb).start()
    lax.fori_loop(1, groups, await_back, 0)

    for c in z_copies + t_copies + list(copies.values()):
        c.wait_send()

    def sent(k, carry):
        for n in range(2):
            two = pl.ds(n * 2, 2)
            remote(codes2.at[0, two], got2.at[0, two], b_send.at[n, k], b_recv.at[n, k], partner).wait_send()
        return carry

    lax.fori_loop(1, groups, sent, 0)

    def sent_first(i, carry):
        first_copy(i).wait_send()
        put(i).wait()
        return carry

    lax.fori_loop(1, 16, sent_first, 0)
    put(0).wait()
    col_copy.wait_send()
    pl.when(s > 0)(to_above.wait_send)
    pl.when(s < 15)(to_below.wait_send)
    pl.when(has_up)(edge_copies[0].wait_send)
    pl.when(has_down)(edge_copies[1].wait_send)


def turn_back(codes, out):
    chans = out.shape[0]
    half = codes.shape[-1]
    slot = (2, 0, 1, 3)

    def some(c, carry):
        part = pl.ds(pl.multiple_of(c * 8, 8), 8)
        for side in range(2):
            lines = [decode(codes[n, side, slot[r], part, :], TOP_E2)[None] for n in range(2) for r in range(4)]
            out[part, :, side * half : (side + 1) * half] = jnp.swapaxes(jnp.concatenate(lines, axis=0), 0, 1)
        return carry

    lax.fori_loop(0, chans // 8, some, 0, unroll=True)


def body(spectrum, land_sea, courant, refract, depth_dx, depth_dy, w_in, w_out):
    freqs, dirs, rows, cols = spectrum.shape
    chans = freqs * dirs
    half = cols // 2
    angles = (np.arange(DIRS, dtype=np.float32) + np.float32(0.5)) * np.float32(2.0 * math.pi / DIRS)
    cos_table = np.ascontiguousarray(np.broadcast_to(np.tile(np.cos(angles), freqs)[:, None], (chans, cols)))
    sin_table = np.ascontiguousarray(np.broadcast_to(np.tile(np.sin(angles), freqs)[:, None], (chans, cols)))
    anywhere = pl.BlockSpec(memory_space=pl.ANY)
    smem = pl.BlockSpec(memory_space=pltpu.SMEM)
    dma = pltpu.SemaphoreType.DMA
    i16, f32, b16 = jnp.int16, jnp.float32, jnp.bfloat16
    back = pl.pallas_call(
        kernel,
        out_shape=jax.ShapeDtypeStruct((16, 4, chans, half), i16),
        in_specs=[anywhere] * 4 + [smem] * 2 + [anywhere] * 4,
        out_specs=anywhere,
        scratch_shapes=[
            pltpu.VMEM((chans, rows, cols), f32),
            pltpu.VMEM((rows, cols), f32),
            pltpu.VMEM((rows, cols), f32),
            pltpu.VMEM((rows, cols), jnp.int32),
            pltpu.VMEM((chans, cols), f32),
            pltpu.VMEM((chans, cols), f32),
            pltpu.VMEM((9, 128, 128), b16),
            pltpu.VMEM((128, 9 * 128), b16),
            pltpu.VMEM((rows + 2, chans, cols), f32),
            pltpu.VMEM((8, cols), f32),
            pltpu.VMEM((9, 128, 128), b16),
            pltpu.VMEM((2, 16, 9, 128, 128), b16),
            pltpu.VMEM((16, 4, chans, half), i16),
            pltpu.VMEM((16, 4, chans, half), i16),
            pltpu.VMEM((16, 4, chans, half), i16),
            pltpu.VMEM((16, 4, chans, half), i16),
            pltpu.VMEM((16, 8, cols), f32),
            pltpu.VMEM((2, 16, chans, half), i16),
            pltpu.VMEM((2, 16, chans, half), i16),
            pltpu.VMEM((chans, half), f32),
            pltpu.VMEM((chans, half), f32),
            pltpu.VMEM((16, 6, chans, half), f32),
            pltpu.VMEM((16, chans, cols), f32),
            pltpu.VMEM((2, 16 * chans, cols), b16),
            pltpu.VMEM((2, 2048, cols), b16),
            pltpu.VMEM((16 * chans, cols), f32),
            pltpu.VMEM((7, chans, cols), f32),
            dma((3,)), dma((3,)), dma((4,)), dma((4,)), dma((4, 4)), dma((4, 4)), dma((4, 4)), dma((4, 4)),
            dma((16,)), dma((16,)), dma((16,)), dma((16,)), dma((2,)), dma((2,)), dma((2, 16)), dma((2, 16)),
            dma((2,)), dma((2,)), dma((1,)), dma((1,)), dma((4,)), dma((4,)), dma((4,)), dma((4,)),
            dma((1,)), dma((8,)), dma((16,)),
        ],
        compiler_params=pltpu.CompilerParams(
            collective_id=0, has_side_effects=True, vmem_limit_bytes=60 * 1024 * 1024
        ),
    )(
        spectrum.reshape(chans, rows, cols), depth_dx, depth_dy, land_sea, courant, refract, cos_table, sin_table,
        w_in.reshape(9, 128, 128), w_out,
    )
    result = pl.pallas_call(
        turn_back,
        grid=(4,),
        out_shape=jax.ShapeDtypeStruct((chans, rows, cols), f32),
        in_specs=[pl.BlockSpec((2, 2, 4, chans, half), lambda i: (i, 0, 0, 0, 0))],
        out_specs=pl.BlockSpec((chans, 8, cols), lambda i: (0, i, 0)),
    )(back.reshape(8, 2, 4, chans, half))
    return result.reshape(freqs, dirs, rows, cols)


def solution(mesh):
    placed = (
        P("freq", None, "space", None),
        P("space", None),
        P("freq"),
        P("freq"),
        P("space", None),
        P("space", None),
        P(None, "freq"),
        P("freq", None),
    )
    return jax.shard_map(
        body, mesh=mesh, in_specs=placed, out_specs=P("freq", None, "space", None), check_vma=False
    )
```

```python
import math

import jax
import jax.numpy as jnp
import numpy as np
from jax import lax
from jax.experimental import pallas as pl
from jax.experimental.pallas import tpu as pltpu
from jax.sharding import PartitionSpec as P

DIRS = 36
MESH = pl.DeviceIdType.MESH

step_scale = 0.5
epsilon = 1e-06

TOP_T1 = 2.45
TOP_E1 = 4.06
TOP_E2 = 8.2
LEVELS = 65535.0
HALF = 32768.0


def encode(value, top):
    level = jnp.minimum(value * (LEVELS / top) + 0.5, LEVELS)
    return (level.astype(jnp.int32) - 32768).astype(jnp.int16)


def decode(code, top):
    return (code.astype(jnp.int32).astype(jnp.float32) + HALF) * (top / LEVELS)


def freq_of(rb, cb):
    high = rb // 4
    yy = rb % 4
    return (yy + high * (3 - 2 * yy)) * 4 + high + cb * 2


def block_of(f):
    y = f // 4
    zl = f % 4
    high = zl % 2
    return high * 4 + y + high * (3 - 2 * y), zl // 2


def coefficients(table, cosine, sine):
    first = lax.broadcasted_iota(jnp.int32, cosine.shape, 0) < DIRS
    courant = jnp.where(first, table[0:1], table[1:2])
    refract = jnp.where(first, table[2:3], table[3:4])
    speed_x = courant * cosine
    speed_y = courant * sine
    pos_x = jnp.maximum(speed_x, 0.0)
    pos_y = jnp.maximum(speed_y, 0.0)
    keep = 1.0 - jnp.abs(speed_x) - jnp.abs(speed_y)
    return keep, pos_x, pos_x - speed_x, pos_y, pos_y - speed_y, refract * sine, refract * cosine


def transport_row(before, center, after, west_edge, east_edge, coef, dx, dy, sea):
    keep, pos_x, neg_x, pos_y, neg_y, turn_x, turn_y = coef
    rows, cols = center.shape
    lane = lax.broadcasted_iota(jnp.int32, center.shape, 1)
    west = jnp.where(lane == 0, west_edge, pltpu.roll(center, 1, 1))
    east = jnp.where(lane == cols - 1, east_edge, pltpu.roll(center, cols - 1, 1))
    shifted = center * keep + pos_x * before + neg_x * after + pos_y * west + neg_y * east
    turning = (turn_x * dx - turn_y * dy) * shifted
    moved_up = jnp.maximum(turning, 0.0)
    moved_down = jnp.maximum(-turning, 0.0)
    d = lax.broadcasted_iota(jnp.int32, center.shape, 0)
    lower = jnp.where((d == 0) | (d == DIRS), pltpu.roll(moved_up, DIRS + 1, 0), pltpu.roll(moved_up, 1, 0))
    upper = jnp.where(
        (d == DIRS - 1) | (d == rows - 1),
        pltpu.roll(moved_down, DIRS - 1, 0),
        pltpu.roll(moved_down, rows - 1, 0),
    )
    return (shifted - jnp.abs(turning) + lower + upper) * sea


def gelu(x):
    near = math.sqrt(2.0 / math.pi)
    part = 0.5 * x
    return part + part * jnp.tanh(x * (near + near * 0.044715 * (x * x)))


def kernel(
    spectrum_in, dx_in, dy_in, land_in, courant, refract, cos_in, sin_in, w_in_in, w_out_in, out,
    spectrum, dx, dy, land, cos_ref, sin_ref, w_in, w_out,
    field, own_table, own_w, weights, codes1, got1, codes2, got2, table, edge_out, edge_in, col_out, col_in,
    energy, moved, x_buf, h_buf, s_buf, coef_buf, coef_all,
    z_send, z_recv, y_send, y_recv, x_send, x_recv, d_send, d_recv, a_send, a_recv, t_send, t_recv,
    e_send, e_recv, b_send, b_recv, halo_send, halo_recv, c_send, c_recv, l_send, l_recv, m_send, m_recv,
    local_sem, load_sem, store_sem,
):
    s = lax.axis_index("space")
    f = lax.axis_index("freq")
    core = s % 2
    x = (s // 2) % 4
    base = (s // 8) * 8
    y = f // 4
    zl = f % 4
    rb, cb = block_of(f)
    chans, rows, cols = spectrum.shape
    half = cols // 2
    groups = 16

    def at_freq(g):
        return {"space": s, "freq": g}

    def at_x(step):
        return {"space": base + ((x + step) % 4) * 2 + core, "freq": f}

    partner = {"space": s + 1 - 2 * core, "freq": f}
    above = {"space": jnp.maximum(s - 1, 0), "freq": f}
    below = {"space": jnp.minimum(s + 1, 15), "freq": f}
    has_up = jnp.logical_or(rb > 0, s > 0)
    has_down = jnp.logical_or(rb < 7, s < 15)
    up = {"space": jnp.where(rb > 0, s, jnp.maximum(s - 1, 0)), "freq": freq_of((rb + 7) % 8, cb)}
    down = {"space": jnp.where(rb < 7, s, jnp.minimum(s + 1, 15)), "freq": freq_of((rb + 1) % 8, cb)}
    beside = at_freq(freq_of(rb, 1 - cb))

    barrier = pltpu.get_barrier_semaphore()

    def greet(target):
        pl.semaphore_signal(barrier, inc=1, device_id=target, device_id_type=MESH)

    for k in range(1, groups):
        greet(at_freq((f + k) % 16))
    greet(at_x(1))
    greet(at_x(3))
    greet(partner)
    over_top = jnp.logical_and(rb == 0, s > 0)
    over_bottom = jnp.logical_and(rb == 7, s < 15)
    other_above = jnp.logical_and(core == 0, s > 0)
    other_below = jnp.logical_and(core == 1, s < 15)
    pl.when(over_top)(lambda: greet(up))
    pl.when(over_bottom)(lambda: greet(down))
    pl.when(other_above)(lambda: greet(above))
    pl.when(other_below)(lambda: greet(below))

    loads = [
        pltpu.make_async_copy(src, dst, load_sem.at[i])
        for i, (src, dst) in enumerate(
            (
                (w_in_in, w_in), (w_out_in, w_out), (spectrum_in, spectrum), (cos_in, cos_ref), (sin_in, sin_ref),
                (dx_in, dx), (dy_in, dy), (land_in, land),
            )
        )
    ]
    for c in loads:
        c.start()
    loads[0].wait()
    loads[1].wait()

    @pl.when(core == 0)
    def _():
        for k in range(9):
            own_w[k] = w_in[k].T

    @pl.when(core == 1)
    def _():
        for k in range(9):
            own_w[k] = w_out[:, k * 128 : (k + 1) * 128].T

    row_of = lax.broadcasted_iota(jnp.int32, (8, cols), 0)
    own_table[...] = jnp.where(
        row_of == 0, courant[0], jnp.where(row_of == 1, courant[1], jnp.where(row_of == 2, refract[0], refract[1]))
    )

    def turn(n):
        def some(c, carry):
            block = spectrum[pl.ds(c * 8, 8), pl.ds(n * 8, 8), :]
            field[pl.ds(n * 8 + 1, 8), pl.ds(pl.multiple_of(c * 8, 8), 8), :] = jnp.swapaxes(block, 0, 1)
            return carry

        lax.fori_loop(0, chans // 8, some, 0)

    loads[2].wait()
    turn(0)
    turn(3)
    known = (over_top, over_bottom, other_above, other_below)
    pl.semaphore_wait(barrier, 18 + sum(k.astype(jnp.int32) for k in known))

    def remote(src, dst, send, recv, target):
        return pltpu.make_async_remote_copy(
            src_ref=src, dst_ref=dst, send_sem=send, recv_sem=recv, device_id=target, device_id_type=MESH
        )

    def quarter(q):
        return pl.ds(pl.multiple_of(q * 32, 32), 32)

    to_above = remote(field.at[1], field.at[rows + 1], halo_send.at[0], halo_recv.at[1], above)
    to_below = remote(field.at[rows], field.at[0], halo_send.at[1], halo_recv.at[0], below)
    pl.when(s > 0)(to_above.start)
    pl.when(s < 15)(to_below.start)
    own_quarter = weights.at[core, f, :, quarter(x), :]
    z_copies = []
    for k in range(1, 4):
        c = remote(
            own_w.at[:, quarter(x), :], own_quarter, z_send.at[k - 1], z_recv.at[k - 1], at_freq(y * 4 + (zl + k) % 4)
        )
        c.start()
        z_copies.append(c)
    place = pltpu.make_async_copy(own_w.at[:, quarter(x), :], own_quarter, local_sem.at[0])
    place.start()
    table[f] = own_table[...]
    t_copies = []
    for k in range(1, groups):
        c = remote(own_table, table.at[f], t_send.at[k], t_recv.at[k], at_freq((f + k) % 16))
        c.start()
        t_copies.append(c)
    turn(1)
    turn(2)
    for c in loads[3:]:
        c.wait()
    place.wait()

    y_right, y_left = at_freq(((y + 1) % 4) * 4 + zl), at_freq(((y + 3) % 4) * 4 + zl)
    order = [y, (y + 3) % 4, (y + 1) % 4, (y + 2) % 4]
    xs = [x, (x + 3) % 4, (x + 1) % 4, (x + 2) % 4]
    whole, front, rear = (0, 9), (0, 5), (5, 4)
    copies = {}

    def by_quarter(b, q, ks=whole):
        return weights.at[core, pl.ds(order[b] * 4, 3), pl.ds(*ks), quarter(q), :]

    def by_piece(b, ks=whole):
        return weights.at[core, order[b] * 4 + 3, pl.ds(*ks)]

    def go(key, block, send, recv, target):
        c = remote(block, block, send, recv, target)
        c.start()
        copies[key] = c

    def got(*key):
        copies[key].wait_recv()

    def spread(b):
        block = by_quarter(b, x)
        go(("x", b, 0), block, x_send.at[b, 0], x_recv.at[b, 0], at_x(1))
        go(("x", b, 1), block, x_send.at[b, 1], x_recv.at[b, 1], at_x(3))
        share(b, 0)

    def share(b, k):
        go(("d", b, k), by_quarter(b, xs[k]), d_send.at[b, k], d_recv.at[b, k], partner)

    def last_quarter(q, ks=whole):
        return weights.at[core, y * 4 + 3, pl.ds(*ks), quarter(q), :]

    def share_last(k):
        go(("d", 4, k), last_quarter(xs[k]), d_send.at[4, k], d_recv.at[4, k], partner)

    def last_1():
        block = last_quarter(x)
        go(("x", 4, 0), block, x_send.at[4, 0], x_recv.at[4, 0], at_x(1))
        go(("x", 4, 1), block, x_send.at[4, 1], x_recv.at[4, 1], at_x(3))
        share_last(0)

    def last_2():
        got("x", 4, 0)
        go(("x", 4, 2), last_quarter(xs[1], front), x_send.at[4, 2], x_recv.at[4, 2], at_x(1))
        got("x", 4, 1)
        go(("x", 4, 3), last_quarter(xs[2], rear), x_send.at[4, 3], x_recv.at[4, 3], at_x(3))
        share_last(1)
        share_last(2)

    def last_3():
        got("x", 4, 2)
        got("x", 4, 3)
        share_last(3)

    def share_piece(b):
        go(("m", b), by_piece(b), m_send.at[b], m_recv.at[b], partner)

    def weights_1():
        for c in z_copies:
            c.wait_recv()
        own = by_quarter(0, x)
        go(("y", 0), own, y_send.at[0], y_recv.at[0], y_right)
        go(("y", 1), own, y_send.at[1], y_recv.at[1], y_left)
        last_1()
        spread(0)

    def weights_2():
        got("y", 0)
        go(("y", 2), by_quarter(1, x, front), y_send.at[2], y_recv.at[2], y_right)
        spread(1)

    def weights_3():
        got("y", 1)
        go(("y", 3), by_quarter(2, x, rear), y_send.at[3], y_recv.at[3], y_left)
        spread(2)

    def weights_4():
        got("y", 2)
        got("y", 3)
        spread(3)

    def weights_5(b):
        got("x", b, 0)
        go(("x", b, 2), by_quarter(b, xs[1], front), x_send.at[b, 2], x_recv.at[b, 2], at_x(1))
        share(b, 1)
        got("x", b, 1)
        go(("x", b, 3), by_quarter(b, xs[2], rear), x_send.at[b, 3], x_recv.at[b, 3], at_x(3))
        share(b, 2)

    def weights_6(b):
        got("x", b, 2)
        got("x", b, 3)
        share(b, 3)

    def pieces_1():
        go(("l", 0), by_piece(0), l_send.at[0], l_recv.at[0], y_right)
        go(("l", 1), by_piece(0), l_send.at[1], l_recv.at[1], y_left)

    def pieces_2():
        got("l", 0)
        go(("l", 2), by_piece(1, front), l_send.at[2], l_recv.at[2], y_right)
        share_piece(1)
        got("l", 1)
        go(("l", 3), by_piece(2, rear), l_send.at[3], l_recv.at[3], y_left)
        share_piece(2)

    def pieces_3():
        got("l", 2)
        got("l", 3)
        share_piece(3)

    coef = coefficients(own_table[...], cos_ref[...], sin_ref[...])
    for i, c in enumerate(coef):
        coef_buf[i] = c

    def first_row(row, carry):
        value = transport_row(
            field[row], field[row + 1], field[row + 2], 0.0, 0.0, [coef_buf[i] for i in range(7)],
            dx[pl.ds(row, 1), :], dy[pl.ds(row, 1), :], land[pl.ds(row, 1), :].astype(jnp.float32),
        )
        code = encode(value, TOP_T1)
        n, r = row // 4, row % 4
        codes1[n * 2, r] = code[:, :half]
        codes1[n * 2 + 1, r] = code[:, half:]
        return carry

    def outer_rows():
        @pl.when(s > 0)
        def _():
            to_below.wait_recv()

        @pl.when(s == 0)
        def _():
            field[0] = jnp.zeros((chans, cols), jnp.float32)

        @pl.when(s < 15)
        def _():
            to_above.wait_recv()

        @pl.when(s == 15)
        def _():
            field[rows + 1] = jnp.zeros((chans, cols), jnp.float32)

        lax.fori_loop(0, 2, lambda n, carry: first_row(n * (rows - 1), carry), 0)

    def first_copy(i):
        ky, kz = i // 4, i % 4
        g = ((y + ky) % 4) * 4 + (zl + kz) % 4
        n, c = block_of(g)
        return remote(codes1.at[n * 2 + c], got1.at[f], a_send.at[i], a_recv.at[i], at_freq(g))

    def first_send(i, carry):
        first_copy(i).start()
        return carry

    def first_arrival(i, carry):
        g = ((y + 4 - i // 4) % 4) * 4 + (zl + 4 - i % 4) % 4
        remote(codes1.at[0], got1.at[g], a_send.at[i], a_recv.at[i], at_freq(g)).wait_recv()
        return carry

    lax.fori_loop(1, 16, first_row, 0)
    weights_1()
    lax.fori_loop(16, rows - 1, first_row, 0)
    outer_rows()
    mine = pltpu.make_async_copy(codes1.at[rb * 2 + cb], got1.at[f], local_sem.at[0])
    mine.start()
    lax.fori_loop(1, 8, first_send, 0)
    lax.fori_loop(12, 16, first_send, 0)
    last_2()
    weights_2()
    weights_3()
    weights_5(0)
    last_3()
    pieces_1()
    lax.fori_loop(8, 12, first_send, 0)
    mine.wait()
    weights_4()
    for k in range(1, groups):
        t_copies[k - 1].wait_recv()

    def all_coefficients(g, carry):
        for i, c in enumerate(coefficients(table[g][:, :half], cos_ref[:, :half], sin_ref[:, :half])):
            coef_all[g, i] = c
        return carry

    lax.fori_loop(0, groups, all_coefficients, 0)
    weights_5(1)
    weights_5(2)
    pieces_2()
    weights_6(0)
    weights_5(3)

    def rows_of(hidden, blocks, size):
        for n, at in enumerate(blocks):
            yield pl.ds(pl.multiple_of(at, size), size), hidden[n * size : (n + 1) * size]

    def first_quarter(q, p):
        pieces = [b * 4 + n for b in range(4) for n in range(3)]
        lhs = jnp.concatenate(
            [jnp.concatenate([weights[0, g, k, quarter(q), :] for k in range(9)], axis=1) for g in pieces], axis=0
        )
        hidden = gelu(jnp.dot(lhs, x_buf[p], preferred_element_type=jnp.float32)).astype(jnp.bfloat16)
        for where, part in rows_of(hidden, [g * 128 + q * 32 for g in pieces], 32):
            h_buf[p, where, :] = part

    def first_rest(p):
        pieces = [b * 4 + 3 for b in range(4)]
        lhs = jnp.concatenate(
            [jnp.concatenate([weights[0, g, k] for k in range(9)], axis=1) for g in pieces], axis=0
        )
        hidden = gelu(jnp.dot(lhs, x_buf[p], preferred_element_type=jnp.float32)).astype(jnp.bfloat16)
        for where, part in rows_of(hidden, [g * 128 for g in pieces], 128):
            h_buf[p, where, :] = part

    def second_layer(p):
        def some(i, carry):
            lhs = jnp.concatenate(
                [
                    jnp.concatenate([weights[1, g, i * 3 + k] for g in range(16)], axis=1)
                    for k in range(3)
                ],
                axis=0,
            )
            s_buf[pl.ds(pl.multiple_of(i * 384, 384), 384), :] = jnp.dot(
                lhs, h_buf[p], preferred_element_type=jnp.float32
            )
            return carry

        lax.fori_loop(0, 3, some, 0)

    def scale_into_x(total, p):
        mean = jnp.sum(total, axis=0, keepdims=True) * (1.0 / 1152.0) + epsilon
        inverse = 1.0 / mean

        def pair(n, carry):
            both = jnp.concatenate([moved[n * 2], moved[n * 2 + 1]], axis=0) * inverse
            x_buf[p, pl.ds(pl.multiple_of(n * 144, 144), 144), :] = both.astype(jnp.bfloat16)
            return carry

        lax.fori_loop(0, 8, pair, 0)

    def growth(g):
        return jnp.exp(step_scale * jnp.tanh(s_buf[pl.ds(pl.multiple_of(g * 72, 8), 72), :]))

    zeros = jnp.zeros((chans, cols), jnp.float32)
    thin = zeros[:, :half]
    lane = lax.broadcasted_iota(jnp.int32, (chans, half), 1)
    edge_lane = (half - 1) * (1 - cb)
    col_copies = [remote(col_out.at[p], col_in.at[p], c_send.at[p], c_recv.at[p], beside) for p in range(2)]

    edge_copies = [
        remote(edge_out.at[0], edge_in.at[1], e_send.at[0], e_recv.at[1], up),
        remote(edge_out.at[1], edge_in.at[0], e_send.at[1], e_recv.at[0], down),
    ]
    lax.fori_loop(1, 16, first_arrival, 0)
    pairs = ((0, 3), (1, 2))

    def both_of(g, pair):
        return decode(jnp.concatenate([got1[g, pair[0]], got1[g, pair[1]]], axis=1), TOP_T1)

    for p in range(2):

        def load(g, total):
            value = both_of(g, pairs[p])
            moved[g] = value
            return total + value

        scale_into_x(lax.fori_loop(0, groups, load, zeros), p)

    def first_layer_of(i):
        for b in range(4):
            got("d", b, i)

        def one(p, carry):
            first_quarter(xs[i], p)
            return carry

        lax.fori_loop(0, 2, one, 0)

    first_layer_of(0)
    pieces_3()
    first_layer_of(1)
    weights_6(1)
    weights_6(2)
    weights_6(3)
    first_layer_of(2)
    for k in range(4):
        got("d", 4, k)
    for b in range(1, 4):
        got("m", b)

    def last_one(p, carry):
        first_rest(p)
        return carry

    lax.fori_loop(0, 2, last_one, 0)
    first_layer_of(3)
    for p, (first, last) in enumerate(pairs):
        second_layer(p)

        def update(g, carry):
            value = both_of(g, pairs[p]) * growth(g)
            energy[g, first + 1] = value[:, :half]
            energy[g, last + 1] = value[:, half:]
            if p == 0:
                code = encode(value, TOP_E1)
                edge_out[0, g] = code[:, :half]
                edge_out[1, g] = code[:, half:]
            return carry

        lax.fori_loop(0, groups, update, 0, unroll=2)
        if p == 0:
            pl.when(has_up)(edge_copies[0].start)
            pl.when(has_down)(edge_copies[1].start)

    for p in (1, 0):

        def pack(g, block):
            for i in range(2):
                at = g * 2 + i
                turned = pltpu.roll(energy[g, pairs[p][i] + 1], (at - edge_lane + half) % half, 1)
                block = jnp.where(lane == at, turned, block)
            return block

        col_out[p] = lax.fori_loop(0, groups, pack, thin, unroll=4)
        col_copies[p].start()

    west_side = cb.astype(jnp.float32)

    def my_half(line):
        return jnp.where(cb == 0, line[:, :half], line[:, half:])


    def fill(present, copy, slot, row):
        @pl.when(present)
        def _():
            copy.wait_recv()

            def some(g, carry):
                energy[g, row] = decode(edge_in[slot, g], TOP_E1)
                return carry

            lax.fori_loop(0, groups, some, 0)

        @pl.when(jnp.logical_not(present))
        def _():
            def some(g, carry):
                energy[g, row] = thin
                return carry

            lax.fori_loop(0, groups, some, 0)

    for n, pair in enumerate(pairs[::-1]):
        col_copies[1 - n].wait_recv()
        if n == 1:
            fill(has_up, edge_copies[1], 0, 0)
            fill(has_down, edge_copies[0], 1, 5)

        def second(g, total):
            coef = [coef_all[g, i] for i in range(7)]
            done = []
            for i, r in enumerate(pair):
                row = pl.ds(rb * 4 + r, 1)
                side = pltpu.roll(col_in[1 - n], (edge_lane - (g * 2 + i) + half) % half, 1)
                done.append(
                    transport_row(
                        energy[g, r], energy[g, r + 1], energy[g, r + 2], side * west_side, side * (1.0 - west_side),
                        coef, my_half(dx[row, :]), my_half(dy[row, :]), my_half(land[row, :]).astype(jnp.float32),
                    )
                )
            value = jnp.concatenate(done, axis=1)
            moved[g] = value
            return total + value

        scale_into_x(lax.fori_loop(0, groups, second, zeros, unroll=2), n)

        def quarters(q, carry):
            first_quarter(q, n)
            return carry

        lax.fori_loop(0, 4, quarters, 0)
        first_rest(n)
        second_layer(n)

        def finish(k):
            g = (f + k) % 16
            code = encode(moved[g] * growth(g), TOP_E2)
            codes2[g, n * 2] = code[:, :half]
            codes2[g, n * 2 + 1] = code[:, half:]

        def finish_and_send(k, carry):
            finish(k)
            g = (f + k) % 16
            two = pl.ds(n * 2, 2)
            remote(codes2.at[g, two], got2.at[rb * 2 + cb, two], b_send.at[n, k], b_recv.at[n, k], at_freq(g)).start()
            return carry

        lax.fori_loop(1, groups, finish_and_send, 0, unroll=3)
        finish(0)

    own_back = pltpu.make_async_copy(codes2.at[f], got2.at[rb * 2 + cb], local_sem.at[0])
    own_back.start()

    def await_back(k, carry):
        g = (f + 16 - k) % 16
        b, c = block_of(g)
        for n in range(2):
            two = pl.ds(n * 2, 2)
            remote(codes2.at[0, two], got2.at[b * 2 + c, two], b_send.at[n, k], b_recv.at[n, k], at_freq(g)).wait_recv()
        put(b * 2 + c).start()
        return carry

    def put(n):
        return pltpu.make_async_copy(got2.at[n], out.at[n], store_sem.at[n])

    own_back.wait()
    put(rb * 2 + cb).start()
    lax.fori_loop(1, groups, await_back, 0)

    for c in z_copies + t_copies + list(copies.values()):
        c.wait_send()

    def sent(k, carry):
        for n in range(2):
            two = pl.ds(n * 2, 2)
            remote(codes2.at[0, two], got2.at[0, two], b_send.at[n, k], b_recv.at[n, k], partner).wait_send()
        return carry

    lax.fori_loop(1, groups, sent, 0)

    def sent_first(i, carry):
        first_copy(i).wait_send()
        put(i).wait()
        return carry

    lax.fori_loop(1, 16, sent_first, 0)
    put(0).wait()
    for c in col_copies:
        c.wait_send()
    pl.when(s > 0)(to_above.wait_send)
    pl.when(s < 15)(to_below.wait_send)
    pl.when(has_up)(edge_copies[0].wait_send)
    pl.when(has_down)(edge_copies[1].wait_send)


def turn_back(codes, out):
    chans = out.shape[0]
    half = codes.shape[-1]
    slot = (2, 0, 1, 3)

    def some(i, carry):
        lines_of = pl.ds(pl.multiple_of(i * 8, 8), 8)
        for c in range(chans // 8):
            part = pl.ds(c * 8, 8)
            for side in range(2):
                lines = [
                    decode(codes[i * 2 + n, side, slot[r], part, :], TOP_E2)[None] for n in range(2) for r in range(4)
                ]
                out[part, lines_of, side * half : (side + 1) * half] = jnp.swapaxes(jnp.concatenate(lines, axis=0), 0, 1)
        return carry

    lax.fori_loop(0, 4, some, 0)


def body(spectrum, land_sea, courant, refract, depth_dx, depth_dy, w_in, w_out):
    freqs, dirs, rows, cols = spectrum.shape
    chans = freqs * dirs
    half = cols // 2
    angles = (np.arange(DIRS, dtype=np.float32) + np.float32(0.5)) * np.float32(2.0 * math.pi / DIRS)
    cos_table = np.ascontiguousarray(np.broadcast_to(np.tile(np.cos(angles), freqs)[:, None], (chans, cols)))
    sin_table = np.ascontiguousarray(np.broadcast_to(np.tile(np.sin(angles), freqs)[:, None], (chans, cols)))
    anywhere = pl.BlockSpec(memory_space=pl.ANY)
    smem = pl.BlockSpec(memory_space=pltpu.SMEM)
    dma = pltpu.SemaphoreType.DMA
    i16, f32, b16 = jnp.int16, jnp.float32, jnp.bfloat16
    back = pl.pallas_call(
        kernel,
        out_shape=jax.ShapeDtypeStruct((16, 4, chans, half), i16),
        in_specs=[anywhere] * 4 + [smem] * 2 + [anywhere] * 4,
        out_specs=anywhere,
        scratch_shapes=[
            pltpu.VMEM((chans, rows, cols), f32),
            pltpu.VMEM((rows, cols), f32),
            pltpu.VMEM((rows, cols), f32),
            pltpu.VMEM((rows, cols), jnp.int32),
            pltpu.VMEM((chans, cols), f32),
            pltpu.VMEM((chans, cols), f32),
            pltpu.VMEM((9, 128, 128), b16),
            pltpu.VMEM((128, 9 * 128), b16),
            pltpu.VMEM((rows + 2, chans, cols), f32),
            pltpu.VMEM((8, cols), f32),
            pltpu.VMEM((9, 128, 128), b16),
            pltpu.VMEM((2, 16, 9, 128, 128), b16),
            pltpu.VMEM((16, 4, chans, half), i16),
            pltpu.VMEM((16, 4, chans, half), i16),
            pltpu.VMEM((16, 4, chans, half), i16),
            pltpu.VMEM((16, 4, chans, half), i16),
            pltpu.VMEM((16, 8, cols), f32),
            pltpu.VMEM((2, 16, chans, half), i16),
            pltpu.VMEM((2, 16, chans, half), i16),
            pltpu.VMEM((2, chans, half), f32),
            pltpu.VMEM((2, chans, half), f32),
            pltpu.VMEM((16, 6, chans, half), f32),
            pltpu.VMEM((16, chans, cols), f32),
            pltpu.VMEM((2, 16 * chans, cols), b16),
            pltpu.VMEM((2, 2048, cols), b16),
            pltpu.VMEM((16 * chans, cols), f32),
            pltpu.VMEM((7, chans, cols), f32),
            pltpu.VMEM((16, 7, chans, half), f32),
            dma((3,)), dma((3,)), dma((4,)), dma((4,)), dma((5, 4)), dma((5, 4)), dma((5, 4)), dma((5, 4)),
            dma((16,)), dma((16,)), dma((16,)), dma((16,)), dma((2,)), dma((2,)), dma((2, 16)), dma((2, 16)),
            dma((2,)), dma((2,)), dma((2,)), dma((2,)), dma((4,)), dma((4,)), dma((4,)), dma((4,)),
            dma((1,)), dma((8,)), dma((16,)),
        ],
        compiler_params=pltpu.CompilerParams(
            collective_id=0, has_side_effects=True, vmem_limit_bytes=60 * 1024 * 1024
        ),
    )(
        spectrum.reshape(chans, rows, cols), depth_dx, depth_dy, land_sea, courant, refract, cos_table, sin_table,
        w_in.reshape(9, 128, 128), w_out,
    )
    result = pl.pallas_call(
        turn_back,
        out_shape=jax.ShapeDtypeStruct((chans, rows, cols), f32),
    )(back.reshape(8, 2, 4, chans, half))
    return result.reshape(freqs, dirs, rows, cols)


def solution(mesh):
    placed = (
        P("freq", None, "space", None),
        P("space", None),
        P("freq"),
        P("freq"),
        P("space", None),
        P("space", None),
        P(None, "freq"),
        P("freq", None),
    )
    return jax.shard_map(
        body, mesh=mesh, in_specs=placed, out_specs=P("freq", None, "space", None), check_vma=False
    )
```

```python
import math

import jax
import jax.numpy as jnp
import numpy as np
from jax import lax
from jax.experimental import pallas as pl
from jax.experimental.pallas import tpu as pltpu
from jax.sharding import PartitionSpec as P

DIRS = 36
MESH = pl.DeviceIdType.MESH

step_scale = 0.5
epsilon = 1e-06

TOP_T1 = 2.45
TOP_E1 = 4.06
TOP_E2 = 8.2
LEVELS = 65535.0
HALF = 32768.0


def encode(value, top):
    level = jnp.minimum(value * (LEVELS / top) + 0.5, LEVELS)
    return (level.astype(jnp.int32) - 32768).astype(jnp.int16)


def decode(code, top):
    return (code.astype(jnp.int32).astype(jnp.float32) + HALF) * (top / LEVELS)


def freq_of(rb, cb):
    high = rb // 4
    yy = rb % 4
    return (yy + high * (3 - 2 * yy)) * 4 + high + cb * 2


def block_of(f):
    y = f // 4
    zl = f % 4
    high = zl % 2
    return high * 4 + y + high * (3 - 2 * y), zl // 2


def coefficients(table, cosine, sine):
    first = lax.broadcasted_iota(jnp.int32, cosine.shape, 0) < DIRS
    courant = jnp.where(first, table[0:1], table[1:2])
    refract = jnp.where(first, table[2:3], table[3:4])
    speed_x = courant * cosine
    speed_y = courant * sine
    pos_x = jnp.maximum(speed_x, 0.0)
    pos_y = jnp.maximum(speed_y, 0.0)
    keep = 1.0 - jnp.abs(speed_x) - jnp.abs(speed_y)
    return keep, pos_x, pos_x - speed_x, pos_y, pos_y - speed_y, refract * sine, refract * cosine


def transport_row(before, center, after, west_edge, east_edge, coef, dx, dy, sea):
    keep, pos_x, neg_x, pos_y, neg_y, turn_x, turn_y = coef
    rows, cols = center.shape
    lane = lax.broadcasted_iota(jnp.int32, center.shape, 1)
    west = jnp.where(lane == 0, west_edge, pltpu.roll(center, 1, 1))
    east = jnp.where(lane == cols - 1, east_edge, pltpu.roll(center, cols - 1, 1))
    shifted = center * keep + pos_x * before + neg_x * after + pos_y * west + neg_y * east
    turning = (turn_x * dx - turn_y * dy) * shifted
    moved_up = jnp.maximum(turning, 0.0)
    moved_down = jnp.maximum(-turning, 0.0)
    d = lax.broadcasted_iota(jnp.int32, center.shape, 0)
    lower = jnp.where((d == 0) | (d == DIRS), pltpu.roll(moved_up, DIRS + 1, 0), pltpu.roll(moved_up, 1, 0))
    upper = jnp.where(
        (d == DIRS - 1) | (d == rows - 1),
        pltpu.roll(moved_down, DIRS - 1, 0),
        pltpu.roll(moved_down, rows - 1, 0),
    )
    return (shifted - jnp.abs(turning) + lower + upper) * sea


def gelu(x):
    near = math.sqrt(2.0 / math.pi)
    part = 0.5 * x
    return part + part * jnp.tanh(x * (near + near * 0.044715 * (x * x)))


def kernel(
    spectrum_in, dx_in, dy_in, land_in, courant, refract, cos_in, sin_in, w_in_in, w_out_in, out,
    spectrum, dx, dy, land, cos_ref, sin_ref, w_in, w_out,
    field, own_table, own_w, weights, codes1, got1, codes2, got2, table, edge_out, edge_in, col_out, col_in,
    energy, moved, x_buf, h_buf, s_buf, coef_buf, coef_all,
    z_send, z_recv, y_send, y_recv, x_send, x_recv, d_send, d_recv, a_send, a_recv, t_send, t_recv,
    e_send, e_recv, b_send, b_recv, halo_send, halo_recv, c_send, c_recv, l_send, l_recv, m_send, m_recv,
    local_sem, load_sem, store_sem,
):
    s = lax.axis_index("space")
    f = lax.axis_index("freq")
    core = s % 2
    x = (s // 2) % 4
    base = (s // 8) * 8
    y = f // 4
    zl = f % 4
    rb, cb = block_of(f)
    chans, rows, cols = spectrum.shape
    half = cols // 2
    groups = 16

    def at_freq(g):
        return {"space": s, "freq": g}

    def at_x(step):
        return {"space": base + ((x + step) % 4) * 2 + core, "freq": f}

    def at_z(step):
        z = ((s // 8) * 4 + zl + step + 8) % 8
        return {"space": (z // 4) * 8 + s % 8, "freq": y * 4 + z % 4}

    partner = {"space": s + 1 - 2 * core, "freq": f}
    above = {"space": jnp.maximum(s - 1, 0), "freq": f}
    below = {"space": jnp.minimum(s + 1, 15), "freq": f}
    has_up = jnp.logical_or(rb > 0, s > 0)
    has_down = jnp.logical_or(rb < 7, s < 15)
    up = {"space": jnp.where(rb > 0, s, jnp.maximum(s - 1, 0)), "freq": freq_of((rb + 7) % 8, cb)}
    down = {"space": jnp.where(rb < 7, s, jnp.minimum(s + 1, 15)), "freq": freq_of((rb + 1) % 8, cb)}
    beside = at_freq(freq_of(rb, 1 - cb))

    barrier = pltpu.get_barrier_semaphore()

    def greet(target):
        pl.semaphore_signal(barrier, inc=1, device_id=target, device_id_type=MESH)

    for k in range(1, groups):
        greet(at_freq((f + k) % 16))
    greet(at_x(1))
    greet(at_x(3))
    greet(partner)
    for step in (1, -1, 2, -2):
        greet(at_z(step))
    over_top = jnp.logical_and(rb == 0, s > 0)
    over_bottom = jnp.logical_and(rb == 7, s < 15)
    other_above = jnp.logical_and(core == 0, s > 0)
    other_below = jnp.logical_and(core == 1, s < 15)
    pl.when(over_top)(lambda: greet(up))
    pl.when(over_bottom)(lambda: greet(down))
    pl.when(other_above)(lambda: greet(above))
    pl.when(other_below)(lambda: greet(below))

    loads = [
        pltpu.make_async_copy(src, dst, load_sem.at[i])
        for i, (src, dst) in enumerate(
            (
                (w_in_in, w_in), (w_out_in, w_out), (spectrum_in, spectrum), (cos_in, cos_ref), (sin_in, sin_ref),
                (dx_in, dx), (dy_in, dy), (land_in, land),
            )
        )
    ]
    for c in loads:
        c.start()
    loads[0].wait()
    loads[1].wait()

    @pl.when(core == 0)
    def _():
        for k in range(9):
            own_w[k] = w_in[k].T

    @pl.when(core == 1)
    def _():
        for k in range(9):
            own_w[k] = w_out[:, k * 128 : (k + 1) * 128].T

    row_of = lax.broadcasted_iota(jnp.int32, (8, cols), 0)
    own_table[...] = jnp.where(
        row_of == 0, courant[0], jnp.where(row_of == 1, courant[1], jnp.where(row_of == 2, refract[0], refract[1]))
    )

    def turn(n):
        def some(c, carry):
            block = spectrum[pl.ds(c * 8, 8), pl.ds(n * 8, 8), :]
            field[pl.ds(n * 8 + 1, 8), pl.ds(pl.multiple_of(c * 8, 8), 8), :] = jnp.swapaxes(block, 0, 1)
            return carry

        lax.fori_loop(0, chans // 8, some, 0)

    loads[2].wait()
    turn(0)
    turn(3)
    known = (over_top, over_bottom, other_above, other_below)
    pl.semaphore_wait(barrier, 22 + sum(k.astype(jnp.int32) for k in known))

    def remote(src, dst, send, recv, target):
        return pltpu.make_async_remote_copy(
            src_ref=src, dst_ref=dst, send_sem=send, recv_sem=recv, device_id=target, device_id_type=MESH
        )

    def quarter(q):
        return pl.ds(pl.multiple_of(q * 32, 32), 32)

    to_above = remote(field.at[1], field.at[rows + 1], halo_send.at[0], halo_recv.at[1], above)
    to_below = remote(field.at[rows], field.at[0], halo_send.at[1], halo_recv.at[0], below)
    pl.when(s > 0)(to_above.start)
    pl.when(s < 15)(to_below.start)
    own_quarter = weights.at[core, f, :, quarter(x), :]
    z_copies = []
    for n, (step, ks) in enumerate(((1, (0, 9)), (-1, (0, 9)), (2, (0, 5)), (-2, (5, 4)))):
        c = remote(
            own_w.at[pl.ds(*ks), quarter(x), :], weights.at[core, f, pl.ds(*ks), quarter(x), :],
            z_send.at[n], z_recv.at[n], at_z(step),
        )
        c.start()
        z_copies.append(c)
    place = pltpu.make_async_copy(own_w.at[:, quarter(x), :], own_quarter, local_sem.at[0])
    place.start()
    table[f] = own_table[...]
    t_copies = []
    for k in range(1, groups):
        c = remote(own_table, table.at[f], t_send.at[k], t_recv.at[k], at_freq((f + k) % 16))
        c.start()
        t_copies.append(c)
    turn(1)
    turn(2)
    for c in loads[3:]:
        c.wait()
    place.wait()

    y_right, y_left = at_freq(((y + 1) % 4) * 4 + zl), at_freq(((y + 3) % 4) * 4 + zl)
    order = [y, (y + 3) % 4, (y + 1) % 4, (y + 2) % 4]
    xs = [x, (x + 3) % 4, (x + 1) % 4, (x + 2) % 4]
    whole, front, rear = (0, 9), (0, 5), (5, 4)
    copies = {}

    def by_quarter(b, q, ks=whole):
        return weights.at[core, pl.ds(order[b] * 4, 3), pl.ds(*ks), quarter(q), :]

    def by_piece(b, ks=whole):
        return weights.at[core, order[b] * 4 + 3, pl.ds(*ks)]

    def go(key, block, send, recv, target):
        c = remote(block, block, send, recv, target)
        c.start()
        copies[key] = c

    def got(*key):
        copies[key].wait_recv()

    def spread(b):
        block = by_quarter(b, x)
        go(("x", b, 0), block, x_send.at[b, 0], x_recv.at[b, 0], at_x(1))
        go(("x", b, 1), block, x_send.at[b, 1], x_recv.at[b, 1], at_x(3))
        share(b, 0)

    def share(b, k):
        go(("d", b, k), by_quarter(b, xs[k]), d_send.at[b, k], d_recv.at[b, k], partner)

    def last_quarter(q, ks=whole):
        return weights.at[core, y * 4 + 3, pl.ds(*ks), quarter(q), :]

    def share_last(k):
        go(("d", 4, k), last_quarter(xs[k]), d_send.at[4, k], d_recv.at[4, k], partner)

    def last_1():
        block = last_quarter(x)
        go(("x", 4, 0), block, x_send.at[4, 0], x_recv.at[4, 0], at_x(1))
        go(("x", 4, 1), block, x_send.at[4, 1], x_recv.at[4, 1], at_x(3))
        share_last(0)

    def last_2():
        got("x", 4, 0)
        go(("x", 4, 2), last_quarter(xs[1], front), x_send.at[4, 2], x_recv.at[4, 2], at_x(1))
        got("x", 4, 1)
        go(("x", 4, 3), last_quarter(xs[2], rear), x_send.at[4, 3], x_recv.at[4, 3], at_x(3))
        share_last(1)
        share_last(2)

    def last_3():
        got("x", 4, 2)
        got("x", 4, 3)
        share_last(3)

    def share_piece(b):
        go(("m", b), by_piece(b), m_send.at[b], m_recv.at[b], partner)

    def weights_1():
        for c in z_copies:
            c.wait_recv()
        own = by_quarter(0, x)
        go(("y", 0), own, y_send.at[0], y_recv.at[0], y_right)
        go(("y", 1), own, y_send.at[1], y_recv.at[1], y_left)
        last_1()
        spread(0)

    def weights_2():
        got("y", 0)
        go(("y", 2), by_quarter(1, x, front), y_send.at[2], y_recv.at[2], y_right)
        spread(1)

    def weights_3():
        got("y", 1)
        go(("y", 3), by_quarter(2, x, rear), y_send.at[3], y_recv.at[3], y_left)
        spread(2)

    def weights_4():
        got("y", 2)
        got("y", 3)
        spread(3)

    def weights_5(b):
        got("x", b, 0)
        go(("x", b, 2), by_quarter(b, xs[1], front), x_send.at[b, 2], x_recv.at[b, 2], at_x(1))
        share(b, 1)
        got("x", b, 1)
        go(("x", b, 3), by_quarter(b, xs[2], rear), x_send.at[b, 3], x_recv.at[b, 3], at_x(3))
        share(b, 2)

    def weights_6(b):
        got("x", b, 2)
        got("x", b, 3)
        share(b, 3)

    def pieces_1():
        go(("l", 0), by_piece(0), l_send.at[0], l_recv.at[0], y_right)
        go(("l", 1), by_piece(0), l_send.at[1], l_recv.at[1], y_left)

    def pieces_2():
        got("l", 0)
        go(("l", 2), by_piece(1, front), l_send.at[2], l_recv.at[2], y_right)
        share_piece(1)
        got("l", 1)
        go(("l", 3), by_piece(2, rear), l_send.at[3], l_recv.at[3], y_left)
        share_piece(2)

    def pieces_3():
        got("l", 2)
        got("l", 3)
        share_piece(3)

    coef = coefficients(own_table[...], cos_ref[...], sin_ref[...])
    for i, c in enumerate(coef):
        coef_buf[i] = c

    def first_row(row, carry):
        value = transport_row(
            field[row], field[row + 1], field[row + 2], 0.0, 0.0, [coef_buf[i] for i in range(7)],
            dx[pl.ds(row, 1), :], dy[pl.ds(row, 1), :], land[pl.ds(row, 1), :].astype(jnp.float32),
        )
        code = encode(value, TOP_T1)
        n, r = row // 4, row % 4
        codes1[n * 2, r] = code[:, :half]
        codes1[n * 2 + 1, r] = code[:, half:]
        return carry

    def outer_rows():
        @pl.when(s > 0)
        def _():
            to_below.wait_recv()

        @pl.when(s == 0)
        def _():
            field[0] = jnp.zeros((chans, cols), jnp.float32)

        @pl.when(s < 15)
        def _():
            to_above.wait_recv()

        @pl.when(s == 15)
        def _():
            field[rows + 1] = jnp.zeros((chans, cols), jnp.float32)

        lax.fori_loop(0, 2, lambda n, carry: first_row(n * (rows - 1), carry), 0)

    def first_copy(i):
        ky, kz = i // 4, i % 4
        g = ((y + ky) % 4) * 4 + (zl + kz) % 4
        n, c = block_of(g)
        return remote(codes1.at[n * 2 + c], got1.at[f], a_send.at[i], a_recv.at[i], at_freq(g))

    def first_send(i, carry):
        first_copy(i).start()
        return carry

    def first_arrival(i, carry):
        g = ((y + 4 - i // 4) % 4) * 4 + (zl + 4 - i % 4) % 4
        remote(codes1.at[0], got1.at[g], a_send.at[i], a_recv.at[i], at_freq(g)).wait_recv()
        return carry

    lax.fori_loop(1, 16, first_row, 0)
    weights_1()
    lax.fori_loop(16, rows - 1, first_row, 0)
    outer_rows()
    mine = pltpu.make_async_copy(codes1.at[rb * 2 + cb], got1.at[f], local_sem.at[0])
    mine.start()
    lax.fori_loop(1, 8, first_send, 0)
    lax.fori_loop(12, 16, first_send, 0)
    last_2()
    weights_2()
    weights_3()
    weights_5(0)
    last_3()
    pieces_1()
    lax.fori_loop(8, 12, first_send, 0)
    mine.wait()
    weights_4()
    for k in range(1, groups):
        t_copies[k - 1].wait_recv()

    def all_coefficients(g, carry):
        for i, c in enumerate(coefficients(table[g][:, :half], cos_ref[:, :half], sin_ref[:, :half])):
            coef_all[g, i] = c
        return carry

    lax.fori_loop(0, groups, all_coefficients, 0)
    weights_5(1)
    weights_5(2)
    pieces_2()
    weights_6(0)
    weights_5(3)

    def rows_of(hidden, blocks, size):
        for n, at in enumerate(blocks):
            yield pl.ds(pl.multiple_of(at, size), size), hidden[n * size : (n + 1) * size]

    def first_quarter(q, p):
        pieces = [b * 4 + n for b in range(4) for n in range(3)]
        lhs = jnp.concatenate(
            [jnp.concatenate([weights[0, g, k, quarter(q), :] for k in range(9)], axis=1) for g in pieces], axis=0
        )
        hidden = gelu(jnp.dot(lhs, x_buf[p], preferred_element_type=jnp.float32)).astype(jnp.bfloat16)
        for where, part in rows_of(hidden, [g * 128 + q * 32 for g in pieces], 32):
            h_buf[p, where, :] = part

    def first_rest(p):
        pieces = [b * 4 + 3 for b in range(4)]
        lhs = jnp.concatenate(
            [jnp.concatenate([weights[0, g, k] for k in range(9)], axis=1) for g in pieces], axis=0
        )
        hidden = gelu(jnp.dot(lhs, x_buf[p], preferred_element_type=jnp.float32)).astype(jnp.bfloat16)
        for where, part in rows_of(hidden, [g * 128 for g in pieces], 128):
            h_buf[p, where, :] = part

    def first_half(i, p):
        lhs = jnp.concatenate(
            [jnp.concatenate([weights[0, i * 8 + n, k] for k in range(9)], axis=1) for n in range(8)], axis=0
        )
        hidden = gelu(jnp.dot(lhs, x_buf[p], preferred_element_type=jnp.float32)).astype(jnp.bfloat16)
        h_buf[p, pl.ds(pl.multiple_of(i * 1024, 1024), 1024), :] = hidden

    def second_part(first, count, p):
        lhs = jnp.concatenate(
            [jnp.concatenate([weights[1, g, first + k] for g in range(16)], axis=1) for k in range(count)], axis=0
        )
        return jnp.dot(lhs, h_buf[p], preferred_element_type=jnp.float32)

    def second_by_parts(p):
        def some(i, carry):
            s_buf[pl.ds(pl.multiple_of(i * 384, 384), 384), :] = second_part(i * 3, 3, p)
            return carry

        lax.fori_loop(0, 3, some, 0)

    def scale_into_x(total, p):
        mean = jnp.sum(total, axis=0, keepdims=True) * (1.0 / 1152.0) + epsilon
        inverse = 1.0 / mean

        def pair(n, carry):
            both = jnp.concatenate([moved[n * 2], moved[n * 2 + 1]], axis=0) * inverse
            x_buf[p, pl.ds(pl.multiple_of(n * 144, 144), 144), :] = both.astype(jnp.bfloat16)
            return carry

        lax.fori_loop(0, 8, pair, 0)

    def growth(g):
        return jnp.exp(step_scale * jnp.tanh(s_buf[pl.ds(pl.multiple_of(g * 72, 8), 72), :]))

    zeros = jnp.zeros((chans, cols), jnp.float32)
    thin = zeros[:, :half]
    lane = lax.broadcasted_iota(jnp.int32, (chans, half), 1)
    edge_lane = (half - 1) * (1 - cb)
    col_copies = [remote(col_out.at[p], col_in.at[p], c_send.at[p], c_recv.at[p], beside) for p in range(2)]

    def edge_copy(side, part):
        some = pl.ds(part * 4, 4 + part * 8)
        return remote(
            edge_out.at[side, some], edge_in.at[1 - side, some], e_send.at[side, part], e_recv.at[1 - side, part],
            up if side == 0 else down,
        )

    edge_copies = [[edge_copy(side, part) for part in range(2)] for side in range(2)]

    def send_edges(part):
        pl.when(has_up)(edge_copies[0][part].start)
        pl.when(has_down)(edge_copies[1][part].start)

    lax.fori_loop(1, 16, first_arrival, 0)
    pairs = ((0, 3), (1, 2))

    def both_of(g, pair):
        return decode(jnp.concatenate([got1[g, pair[0]], got1[g, pair[1]]], axis=1), TOP_T1)

    for p in range(2):

        def load(g, total):
            value = both_of(g, pairs[p])
            moved[g] = value
            return total + value

        scale_into_x(lax.fori_loop(0, groups, load, zeros), p)

    def first_layer_of(i):
        for b in range(4):
            got("d", b, i)

        def one(p, carry):
            first_quarter(xs[i], p)
            return carry

        lax.fori_loop(0, 2, one, 0)

    first_layer_of(0)
    pieces_3()
    first_layer_of(1)
    weights_6(1)
    weights_6(2)
    weights_6(3)
    first_layer_of(2)
    for k in range(4):
        got("d", 4, k)
    for b in range(1, 4):
        got("m", b)

    def last_one(p, carry):
        first_rest(p)
        return carry

    lax.fori_loop(0, 2, last_one, 0)
    first_layer_of(3)
    for p, (first, last) in enumerate(pairs):
        second_by_parts(p)

        def update(g, carry):
            value = both_of(g, pairs[p]) * growth(g)
            energy[g, first + 1] = value[:, :half]
            energy[g, last + 1] = value[:, half:]
            if p == 0:
                code = encode(value, TOP_E1)
                edge_out[0, g] = code[:, :half]
                edge_out[1, g] = code[:, half:]
            return carry

        lax.fori_loop(0, groups, update, 0, unroll=2)
        if p == 0:
            send_edges(0)

    for p in (1, 0):

        def pack(g, block):
            for i in range(2):
                at = g * 2 + i
                turned = pltpu.roll(energy[g, pairs[p][i] + 1], (at - edge_lane + half) % half, 1)
                block = jnp.where(lane == at, turned, block)
            return block

        col_out[p] = lax.fori_loop(0, groups, pack, thin, unroll=4)
        col_copies[p].start()
        if p == 1:
            send_edges(1)

    west_side = cb.astype(jnp.float32)

    def my_half(line):
        return jnp.where(cb == 0, line[:, :half], line[:, half:])


    def fill(present, copies_in, slot, row):
        @pl.when(present)
        def _():
            for c in copies_in:
                c.wait_recv()

            def some(g, carry):
                energy[g, row] = decode(edge_in[slot, g], TOP_E1)
                return carry

            lax.fori_loop(0, groups, some, 0)

        @pl.when(jnp.logical_not(present))
        def _():
            def some(g, carry):
                energy[g, row] = thin
                return carry

            lax.fori_loop(0, groups, some, 0)

    for n, pair in enumerate(pairs[::-1]):
        col_copies[1 - n].wait_recv()
        if n == 1:
            fill(has_up, edge_copies[1], 0, 0)
            fill(has_down, edge_copies[0], 1, 5)

        def second(g, total):
            coef = [coef_all[g, i] for i in range(7)]
            done = []
            for i, r in enumerate(pair):
                row = pl.ds(rb * 4 + r, 1)
                side = pltpu.roll(col_in[1 - n], (edge_lane - (g * 2 + i) + half) % half, 1)
                done.append(
                    transport_row(
                        energy[g, r], energy[g, r + 1], energy[g, r + 2], side * west_side, side * (1.0 - west_side),
                        coef, my_half(dx[row, :]), my_half(dy[row, :]), my_half(land[row, :]).astype(jnp.float32),
                    )
                )
            value = jnp.concatenate(done, axis=1)
            moved[g] = value
            return total + value

        scale_into_x(lax.fori_loop(0, groups, second, zeros, unroll=2), n)

        def halves(i, carry):
            first_half(i, n)
            return carry

        lax.fori_loop(0, 2, halves, 0)
        s_buf[...] = second_part(0, 9, n)

        def finish(k):
            g = (f + k) % 16
            code = encode(moved[g] * growth(g), TOP_E2)
            codes2[g, n * 2] = code[:, :half]
            codes2[g, n * 2 + 1] = code[:, half:]

        def finish_and_send(k, carry):
            finish(k)
            g = (f + k) % 16
            two = pl.ds(n * 2, 2)
            remote(codes2.at[g, two], got2.at[rb * 2 + cb, two], b_send.at[n, k], b_recv.at[n, k], at_freq(g)).start()
            return carry

        lax.fori_loop(1, groups, finish_and_send, 0, unroll=3)
        finish(0)

    own_back = pltpu.make_async_copy(codes2.at[f], got2.at[rb * 2 + cb], local_sem.at[0])
    own_back.start()

    def await_back(k, carry):
        g = (f + 16 - k) % 16
        b, c = block_of(g)
        for n in range(2):
            two = pl.ds(n * 2, 2)
            remote(codes2.at[0, two], got2.at[b * 2 + c, two], b_send.at[n, k], b_recv.at[n, k], at_freq(g)).wait_recv()
        put(b * 2 + c).start()
        return carry

    def put(n):
        return pltpu.make_async_copy(got2.at[n], out.at[n], store_sem.at[n])

    own_back.wait()
    put(rb * 2 + cb).start()
    lax.fori_loop(1, groups, await_back, 0)

    for c in z_copies + t_copies + list(copies.values()):
        c.wait_send()

    def sent(k, carry):
        for n in range(2):
            two = pl.ds(n * 2, 2)
            remote(codes2.at[0, two], got2.at[0, two], b_send.at[n, k], b_recv.at[n, k], partner).wait_send()
        return carry

    lax.fori_loop(1, groups, sent, 0)

    def sent_first(i, carry):
        first_copy(i).wait_send()
        put(i).wait()
        return carry

    lax.fori_loop(1, 16, sent_first, 0)
    put(0).wait()
    for c in col_copies:
        c.wait_send()
    pl.when(s > 0)(to_above.wait_send)
    pl.when(s < 15)(to_below.wait_send)
    for part in range(2):
        pl.when(has_up)(edge_copies[0][part].wait_send)
        pl.when(has_down)(edge_copies[1][part].wait_send)


def turn_back(codes, out):
    chans = out.shape[0]
    half = codes.shape[-1]
    slot = (2, 0, 1, 3)

    def some(i, carry):
        lines_of = pl.ds(pl.multiple_of(i * 8, 8), 8)
        for c in range(chans // 8):
            part = pl.ds(c * 8, 8)
            for side in range(2):
                lines = [
                    decode(codes[i * 2 + n, side, slot[r], part, :], TOP_E2)[None] for n in range(2) for r in range(4)
                ]
                out[part, lines_of, side * half : (side + 1) * half] = jnp.swapaxes(jnp.concatenate(lines, axis=0), 0, 1)
        return carry

    lax.fori_loop(0, 4, some, 0)


def body(spectrum, land_sea, courant, refract, depth_dx, depth_dy, w_in, w_out):
    freqs, dirs, rows, cols = spectrum.shape
    chans = freqs * dirs
    half = cols // 2
    angles = (np.arange(DIRS, dtype=np.float32) + np.float32(0.5)) * np.float32(2.0 * math.pi / DIRS)
    cos_table = np.ascontiguousarray(np.broadcast_to(np.tile(np.cos(angles), freqs)[:, None], (chans, cols)))
    sin_table = np.ascontiguousarray(np.broadcast_to(np.tile(np.sin(angles), freqs)[:, None], (chans, cols)))
    anywhere = pl.BlockSpec(memory_space=pl.ANY)
    smem = pl.BlockSpec(memory_space=pltpu.SMEM)
    dma = pltpu.SemaphoreType.DMA
    i16, f32, b16 = jnp.int16, jnp.float32, jnp.bfloat16
    back = pl.pallas_call(
        kernel,
        out_shape=jax.ShapeDtypeStruct((16, 4, chans, half), i16),
        in_specs=[anywhere] * 4 + [smem] * 2 + [anywhere] * 4,
        out_specs=anywhere,
        scratch_shapes=[
            pltpu.VMEM((chans, rows, cols), f32),
            pltpu.VMEM((rows, cols), f32),
            pltpu.VMEM((rows, cols), f32),
            pltpu.VMEM((rows, cols), jnp.int32),
            pltpu.VMEM((chans, cols), f32),
            pltpu.VMEM((chans, cols), f32),
            pltpu.VMEM((9, 128, 128), b16),
            pltpu.VMEM((128, 9 * 128), b16),
            pltpu.VMEM((rows + 2, chans, cols), f32),
            pltpu.VMEM((8, cols), f32),
            pltpu.VMEM((9, 128, 128), b16),
            pltpu.VMEM((2, 16, 9, 128, 128), b16),
            pltpu.VMEM((16, 4, chans, half), i16),
            pltpu.VMEM((16, 4, chans, half), i16),
            pltpu.VMEM((16, 4, chans, half), i16),
            pltpu.VMEM((16, 4, chans, half), i16),
            pltpu.VMEM((16, 8, cols), f32),
            pltpu.VMEM((2, 16, chans, half), i16),
            pltpu.VMEM((2, 16, chans, half), i16),
            pltpu.VMEM((2, chans, half), f32),
            pltpu.VMEM((2, chans, half), f32),
            pltpu.VMEM((16, 6, chans, half), f32),
            pltpu.VMEM((16, chans, cols), f32),
            pltpu.VMEM((2, 16 * chans, cols), b16),
            pltpu.VMEM((2, 2048, cols), b16),
            pltpu.VMEM((16 * chans, cols), f32),
            pltpu.VMEM((7, chans, cols), f32),
            pltpu.VMEM((16, 7, chans, half), f32),
            dma((4,)), dma((4,)), dma((4,)), dma((4,)), dma((5, 4)), dma((5, 4)), dma((5, 4)), dma((5, 4)),
            dma((16,)), dma((16,)), dma((16,)), dma((16,)), dma((2, 2)), dma((2, 2)), dma((2, 16)), dma((2, 16)),
            dma((2,)), dma((2,)), dma((2,)), dma((2,)), dma((4,)), dma((4,)), dma((4,)), dma((4,)),
            dma((1,)), dma((8,)), dma((16,)),
        ],
        compiler_params=pltpu.CompilerParams(
            collective_id=0, has_side_effects=True, vmem_limit_bytes=60 * 1024 * 1024
        ),
    )(
        spectrum.reshape(chans, rows, cols), depth_dx, depth_dy, land_sea, courant, refract, cos_table, sin_table,
        w_in.reshape(9, 128, 128), w_out,
    )
    result = pl.pallas_call(
        turn_back,
        out_shape=jax.ShapeDtypeStruct((chans, rows, cols), f32),
    )(back.reshape(8, 2, 4, chans, half))
    return result.reshape(freqs, dirs, rows, cols)


def solution(mesh):
    placed = (
        P("freq", None, "space", None),
        P("space", None),
        P("freq"),
        P("freq"),
        P("space", None),
        P("space", None),
        P(None, "freq"),
        P("freq", None),
    )
    return jax.shard_map(
        body, mesh=mesh, in_specs=placed, out_specs=P("freq", None, "space", None), check_vma=False
    )
```

```python
import math

import jax
import jax.numpy as jnp
import numpy as np
from jax import lax
from jax.experimental import pallas as pl
from jax.experimental.pallas import tpu as pltpu
from jax.sharding import PartitionSpec as P

DIRS = 36
MESH = pl.DeviceIdType.MESH

step_scale = 0.5
epsilon = 1e-06

TOP_T1 = 2.45
TOP_E1 = 4.06
TOP_E2 = 8.2
LEVELS = 65535.0
HALF = 32768.0


def encode(value, top):
    level = jnp.minimum(value * (LEVELS / top) + 0.5, LEVELS)
    return (level.astype(jnp.int32) - 32768).astype(jnp.int16)


def decode(code, top):
    return (code.astype(jnp.int32).astype(jnp.float32) + HALF) * (top / LEVELS)


def freq_of(rb, cb):
    high = rb // 4
    yy = rb % 4
    return (yy + high * (3 - 2 * yy)) * 4 + high + cb * 2


def block_of(f):
    y = f // 4
    zl = f % 4
    high = zl % 2
    return high * 4 + y + high * (3 - 2 * y), zl // 2


def coefficients(table, cosine, sine):
    first = lax.broadcasted_iota(jnp.int32, cosine.shape, 0) < DIRS
    courant = jnp.where(first, table[0:1], table[1:2])
    refract = jnp.where(first, table[2:3], table[3:4])
    speed_x = courant * cosine
    speed_y = courant * sine
    pos_x = jnp.maximum(speed_x, 0.0)
    pos_y = jnp.maximum(speed_y, 0.0)
    keep = 1.0 - jnp.abs(speed_x) - jnp.abs(speed_y)
    return keep, pos_x, pos_x - speed_x, pos_y, pos_y - speed_y, refract * sine, refract * cosine


def transport_row(before, center, after, west_edge, east_edge, coef, dx, dy, sea):
    keep, pos_x, neg_x, pos_y, neg_y, turn_x, turn_y = coef
    rows, cols = center.shape
    lane = lax.broadcasted_iota(jnp.int32, center.shape, 1)
    west = jnp.where(lane == 0, west_edge, pltpu.roll(center, 1, 1))
    east = jnp.where(lane == cols - 1, east_edge, pltpu.roll(center, cols - 1, 1))
    shifted = center * keep + pos_x * before + neg_x * after + pos_y * west + neg_y * east
    turning = (turn_x * dx - turn_y * dy) * shifted
    moved_up = jnp.maximum(turning, 0.0)
    moved_down = jnp.maximum(-turning, 0.0)
    d = lax.broadcasted_iota(jnp.int32, center.shape, 0)
    lower = jnp.where((d == 0) | (d == DIRS), pltpu.roll(moved_up, DIRS + 1, 0), pltpu.roll(moved_up, 1, 0))
    upper = jnp.where(
        (d == DIRS - 1) | (d == rows - 1),
        pltpu.roll(moved_down, DIRS - 1, 0),
        pltpu.roll(moved_down, rows - 1, 0),
    )
    return (shifted - jnp.abs(turning) + lower + upper) * sea


def gelu(x):
    near = math.sqrt(2.0 / math.pi)
    part = 0.5 * x
    return part + part * jnp.tanh(x * (near + near * 0.044715 * (x * x)))


def kernel(
    spectrum_in, dx_in, dy_in, land_in, courant, refract, cos_in, sin_in, w_in_in, w_out_in, out,
    spectrum, dx, dy, land, cos_ref, sin_ref, w_in, w_out,
    field, own_table, own_w, weights, codes1, got1, codes2, got2, table, edge_out, edge_in, col_out, col_in,
    energy, moved, x_buf, h_buf, s_buf, coef_buf, coef_all,
    z_send, z_recv, y_send, y_recv, x_send, x_recv, d_send, d_recv, a_send, a_recv, t_send, t_recv,
    e_send, e_recv, b_send, b_recv, halo_send, halo_recv, c_send, c_recv, l_send, l_recv, m_send, m_recv,
    local_sem, load_sem, store_sem,
):
    s = lax.axis_index("space")
    f = lax.axis_index("freq")
    core = s % 2
    x = (s // 2) % 4
    base = (s // 8) * 8
    y = f // 4
    zl = f % 4
    rb, cb = block_of(f)
    chans, rows, cols = spectrum.shape
    half = cols // 2
    groups = 16

    def at_freq(g):
        return {"space": s, "freq": g}

    def at_x(step):
        return {"space": base + ((x + step) % 4) * 2 + core, "freq": f}

    def at_z(step):
        z = ((s // 8) * 4 + zl + step + 8) % 8
        return {"space": (z // 4) * 8 + s % 8, "freq": y * 4 + z % 4}

    partner = {"space": s + 1 - 2 * core, "freq": f}
    above = {"space": jnp.maximum(s - 1, 0), "freq": f}
    below = {"space": jnp.minimum(s + 1, 15), "freq": f}
    has_up = jnp.logical_or(rb > 0, s > 0)
    has_down = jnp.logical_or(rb < 7, s < 15)
    up = {"space": jnp.where(rb > 0, s, jnp.maximum(s - 1, 0)), "freq": freq_of((rb + 7) % 8, cb)}
    down = {"space": jnp.where(rb < 7, s, jnp.minimum(s + 1, 15)), "freq": freq_of((rb + 1) % 8, cb)}
    beside = at_freq(freq_of(rb, 1 - cb))

    barrier = pltpu.get_barrier_semaphore()

    def greet(target):
        pl.semaphore_signal(barrier, inc=1, device_id=target, device_id_type=MESH)

    for k in range(1, groups):
        greet(at_freq((f + k) % 16))
    greet(at_x(1))
    greet(at_x(3))
    greet(partner)
    for step in (1, -1, 2, -2):
        greet(at_z(step))
    over_top = jnp.logical_and(rb == 0, s > 0)
    over_bottom = jnp.logical_and(rb == 7, s < 15)
    other_above = jnp.logical_and(core == 0, s > 0)
    other_below = jnp.logical_and(core == 1, s < 15)
    pl.when(over_top)(lambda: greet(up))
    pl.when(over_bottom)(lambda: greet(down))
    pl.when(other_above)(lambda: greet(above))
    pl.when(other_below)(lambda: greet(below))

    loads = [
        pltpu.make_async_copy(src, dst, load_sem.at[i])
        for i, (src, dst) in enumerate(
            (
                (w_in_in, w_in), (w_out_in, w_out), (spectrum_in, spectrum), (cos_in, cos_ref), (sin_in, sin_ref),
                (dx_in, dx), (dy_in, dy), (land_in, land),
            )
        )
    ]
    for c in loads:
        c.start()
    loads[0].wait()
    loads[1].wait()

    @pl.when(core == 0)
    def _():
        for k in range(9):
            own_w[k] = w_in[k].T

    @pl.when(core == 1)
    def _():
        for k in range(9):
            own_w[k] = w_out[:, k * 128 : (k + 1) * 128].T

    row_of = lax.broadcasted_iota(jnp.int32, (8, cols), 0)
    own_table[...] = jnp.where(
        row_of == 0, courant[0], jnp.where(row_of == 1, courant[1], jnp.where(row_of == 2, refract[0], refract[1]))
    )

    def turn(n):
        def some(c, carry):
            block = spectrum[pl.ds(c * 8, 8), pl.ds(n * 8, 8), :]
            field[pl.ds(n * 8 + 1, 8), pl.ds(pl.multiple_of(c * 8, 8), 8), :] = jnp.swapaxes(block, 0, 1)
            return carry

        lax.fori_loop(0, chans // 8, some, 0)

    loads[2].wait()
    turn(0)
    turn(3)
    known = (over_top, over_bottom, other_above, other_below)
    pl.semaphore_wait(barrier, 22 + sum(k.astype(jnp.int32) for k in known))

    def remote(src, dst, send, recv, target):
        return pltpu.make_async_remote_copy(
            src_ref=src, dst_ref=dst, send_sem=send, recv_sem=recv, device_id=target, device_id_type=MESH
        )

    def quarter(q):
        return pl.ds(pl.multiple_of(q * 32, 32), 32)

    to_above = remote(field.at[1], field.at[rows + 1], halo_send.at[0], halo_recv.at[1], above)
    to_below = remote(field.at[rows], field.at[0], halo_send.at[1], halo_recv.at[0], below)
    pl.when(s > 0)(to_above.start)
    pl.when(s < 15)(to_below.start)
    own_quarter = weights.at[core, f, :, quarter(x), :]
    z_copies = []
    for n, (step, ks) in enumerate(((1, (0, 9)), (-1, (0, 9)), (2, (0, 5)), (-2, (5, 4)))):
        c = remote(
            own_w.at[pl.ds(*ks), quarter(x), :], weights.at[core, f, pl.ds(*ks), quarter(x), :],
            z_send.at[n], z_recv.at[n], at_z(step),
        )
        c.start()
        z_copies.append(c)
    place = pltpu.make_async_copy(own_w.at[:, quarter(x), :], own_quarter, local_sem.at[0])
    place.start()
    table[f] = own_table[...]
    t_copies = []
    for k in range(1, groups):
        c = remote(own_table, table.at[f], t_send.at[k], t_recv.at[k], at_freq((f + k) % 16))
        c.start()
        t_copies.append(c)
    turn(1)
    turn(2)
    for c in loads[3:]:
        c.wait()
    place.wait()

    y_right, y_left = at_freq(((y + 1) % 4) * 4 + zl), at_freq(((y + 3) % 4) * 4 + zl)
    order = [y, (y + 3) % 4, (y + 1) % 4, (y + 2) % 4]
    xs = [x, (x + 3) % 4, (x + 1) % 4, (x + 2) % 4]
    whole, front, rear = (0, 9), (0, 5), (5, 4)
    copies = {}

    def by_quarter(b, q, ks=whole):
        return weights.at[core, pl.ds(order[b] * 4, 3), pl.ds(*ks), quarter(q), :]

    def by_piece(b, ks=whole):
        return weights.at[core, order[b] * 4 + 3, pl.ds(*ks)]

    def go(key, block, send, recv, target):
        c = remote(block, block, send, recv, target)
        c.start()
        copies[key] = c

    def got(*key):
        copies[key].wait_recv()

    def spread(b):
        block = by_quarter(b, x)
        go(("x", b, 0), block, x_send.at[b, 0], x_recv.at[b, 0], at_x(1))
        go(("x", b, 1), block, x_send.at[b, 1], x_recv.at[b, 1], at_x(3))
        share(b, 0)

    def share(b, k):
        go(("d", b, k), by_quarter(b, xs[k]), d_send.at[b, k], d_recv.at[b, k], partner)

    def last_quarter(q, ks=whole):
        return weights.at[core, y * 4 + 3, pl.ds(*ks), quarter(q), :]

    def share_last(k):
        go(("d", 4, k), last_quarter(xs[k]), d_send.at[4, k], d_recv.at[4, k], partner)

    def last_1():
        block = last_quarter(x)
        go(("x", 4, 0), block, x_send.at[4, 0], x_recv.at[4, 0], at_x(1))
        go(("x", 4, 1), block, x_send.at[4, 1], x_recv.at[4, 1], at_x(3))
        share_last(0)

    def last_2():
        got("x", 4, 0)
        go(("x", 4, 2), last_quarter(xs[1], front), x_send.at[4, 2], x_recv.at[4, 2], at_x(1))
        got("x", 4, 1)
        go(("x", 4, 3), last_quarter(xs[2], rear), x_send.at[4, 3], x_recv.at[4, 3], at_x(3))
        share_last(1)
        share_last(2)

    def last_3():
        got("x", 4, 2)
        got("x", 4, 3)
        share_last(3)

    def share_piece(b):
        go(("m", b), by_piece(b), m_send.at[b], m_recv.at[b], partner)

    def weights_1():
        for c in z_copies:
            c.wait_recv()
        own = by_quarter(0, x)
        go(("y", 0), own, y_send.at[0], y_recv.at[0], y_right)
        go(("y", 1), own, y_send.at[1], y_recv.at[1], y_left)
        last_1()
        spread(0)

    def weights_2():
        got("y", 0)
        go(("y", 2), by_quarter(1, x, front), y_send.at[2], y_recv.at[2], y_right)
        spread(1)

    def weights_3():
        got("y", 1)
        go(("y", 3), by_quarter(2, x, rear), y_send.at[3], y_recv.at[3], y_left)
        spread(2)

    def weights_4():
        got("y", 2)
        got("y", 3)
        spread(3)

    def weights_5(b):
        got("x", b, 0)
        go(("x", b, 2), by_quarter(b, xs[1], front), x_send.at[b, 2], x_recv.at[b, 2], at_x(1))
        share(b, 1)
        got("x", b, 1)
        go(("x", b, 3), by_quarter(b, xs[2], rear), x_send.at[b, 3], x_recv.at[b, 3], at_x(3))
        share(b, 2)

    def weights_6(b):
        got("x", b, 2)
        got("x", b, 3)
        share(b, 3)

    def pieces_1():
        go(("l", 0), by_piece(0), l_send.at[0], l_recv.at[0], y_right)
        go(("l", 1), by_piece(0), l_send.at[1], l_recv.at[1], y_left)

    def pieces_2():
        got("l", 0)
        go(("l", 2), by_piece(1, front), l_send.at[2], l_recv.at[2], y_right)
        share_piece(1)
        got("l", 1)
        go(("l", 3), by_piece(2, rear), l_send.at[3], l_recv.at[3], y_left)
        share_piece(2)

    def pieces_3():
        got("l", 2)
        got("l", 3)
        share_piece(3)

    coef = coefficients(own_table[...], cos_ref[...], sin_ref[...])
    for i, c in enumerate(coef):
        coef_buf[i] = c

    def first_row(row, carry):
        value = transport_row(
            field[row], field[row + 1], field[row + 2], 0.0, 0.0, [coef_buf[i] for i in range(7)],
            dx[pl.ds(row, 1), :], dy[pl.ds(row, 1), :], land[pl.ds(row, 1), :].astype(jnp.float32),
        )
        code = encode(value, TOP_T1)
        n, r = row // 4, row % 4
        codes1[n * 2, r] = code[:, :half]
        codes1[n * 2 + 1, r] = code[:, half:]
        return carry

    def outer_rows():
        @pl.when(s > 0)
        def _():
            to_below.wait_recv()

        @pl.when(s == 0)
        def _():
            field[0] = jnp.zeros((chans, cols), jnp.float32)

        @pl.when(s < 15)
        def _():
            to_above.wait_recv()

        @pl.when(s == 15)
        def _():
            field[rows + 1] = jnp.zeros((chans, cols), jnp.float32)

        lax.fori_loop(0, 2, lambda n, carry: first_row(n * (rows - 1), carry), 0)

    def first_copy(i):
        ky, kz = i // 4, i % 4
        g = ((y + ky) % 4) * 4 + (zl + kz) % 4
        n, c = block_of(g)
        return remote(codes1.at[n * 2 + c], got1.at[f], a_send.at[i], a_recv.at[i], at_freq(g))

    def first_send(i, carry):
        first_copy(i).start()
        return carry

    def first_arrival(i, carry):
        g = ((y + 4 - i // 4) % 4) * 4 + (zl + 4 - i % 4) % 4
        remote(codes1.at[0], got1.at[g], a_send.at[i], a_recv.at[i], at_freq(g)).wait_recv()
        return carry

    lax.fori_loop(1, 16, first_row, 0)
    weights_1()
    lax.fori_loop(16, rows - 1, first_row, 0)
    outer_rows()
    mine = pltpu.make_async_copy(codes1.at[rb * 2 + cb], got1.at[f], local_sem.at[0])
    mine.start()
    lax.fori_loop(1, 8, first_send, 0)
    lax.fori_loop(12, 16, first_send, 0)
    last_2()
    weights_2()
    weights_3()
    weights_5(0)
    last_3()
    pieces_1()
    lax.fori_loop(8, 12, first_send, 0)
    mine.wait()
    weights_4()
    for k in range(1, groups):
        t_copies[k - 1].wait_recv()

    def all_coefficients(g, carry):
        for i, c in enumerate(coefficients(table[g][:, :half], cos_ref[:, :half], sin_ref[:, :half])):
            coef_all[g, i] = c
        return carry

    lax.fori_loop(0, groups, all_coefficients, 0)
    weights_5(1)
    weights_5(2)
    pieces_2()
    weights_6(0)
    weights_5(3)

    def first_some(quarters, rest, p):
        pieces = [b * 4 + n for b in range(4) for n in range(3)]
        parts = [(g, quarter(q), g * 128 + q * 32, 32) for q in quarters for g in pieces]
        if rest:
            parts += [(b * 4 + 3, pl.ds(0, 128), b * 512 + 384, 128) for b in range(4)]
        lhs = jnp.concatenate(
            [jnp.concatenate([weights[0, g, k, some, :] for k in range(9)], axis=1) for g, some, _, _ in parts], axis=0
        )
        hidden = gelu(jnp.dot(lhs, x_buf[p], preferred_element_type=jnp.float32)).astype(jnp.bfloat16)
        at = 0
        for _, _, place_row, size in parts:
            h_buf[p, pl.ds(pl.multiple_of(place_row, size), size), :] = hidden[at : at + size]
            at += size

    def first_half(i, p):
        lhs = jnp.concatenate(
            [jnp.concatenate([weights[0, i * 8 + n, k] for k in range(9)], axis=1) for n in range(8)], axis=0
        )
        hidden = gelu(jnp.dot(lhs, x_buf[p], preferred_element_type=jnp.float32)).astype(jnp.bfloat16)
        h_buf[p, pl.ds(pl.multiple_of(i * 1024, 1024), 1024), :] = hidden

    def second_part(first, count, p):
        lhs = jnp.concatenate(
            [jnp.concatenate([weights[1, g, first + k] for g in range(16)], axis=1) for k in range(count)], axis=0
        )
        return jnp.dot(lhs, h_buf[p], preferred_element_type=jnp.float32)

    def second_by_parts(p):
        def some(i, carry):
            s_buf[pl.ds(pl.multiple_of(i * 384, 384), 384), :] = second_part(i * 3, 3, p)
            return carry

        lax.fori_loop(0, 3, some, 0)

    def scale_into_x(total, p):
        mean = jnp.sum(total, axis=0, keepdims=True) * (1.0 / 1152.0) + epsilon
        inverse = 1.0 / mean

        def pair(n, carry):
            both = jnp.concatenate([moved[n * 2], moved[n * 2 + 1]], axis=0) * inverse
            x_buf[p, pl.ds(pl.multiple_of(n * 144, 144), 144), :] = both.astype(jnp.bfloat16)
            return carry

        lax.fori_loop(0, 8, pair, 0)

    def growth(g):
        return jnp.exp(step_scale * jnp.tanh(s_buf[pl.ds(pl.multiple_of(g * 72, 8), 72), :]))

    zeros = jnp.zeros((chans, cols), jnp.float32)
    thin = zeros[:, :half]
    lane = lax.broadcasted_iota(jnp.int32, (chans, half), 1)
    edge_lane = (half - 1) * (1 - cb)
    col_copies = [remote(col_out.at[p], col_in.at[p], c_send.at[p], c_recv.at[p], beside) for p in range(2)]

    def edge_copy(side, part):
        some = pl.ds(part * 4, 4 + part * 8)
        return remote(
            edge_out.at[side, some], edge_in.at[1 - side, some], e_send.at[side, part], e_recv.at[1 - side, part],
            up if side == 0 else down,
        )

    edge_copies = [[edge_copy(side, part) for part in range(2)] for side in range(2)]

    def send_edges(part):
        pl.when(has_up)(edge_copies[0][part].start)
        pl.when(has_down)(edge_copies[1][part].start)

    lax.fori_loop(1, 16, first_arrival, 0)
    pairs = ((0, 3), (1, 2))

    def both_of(g, pair):
        return decode(jnp.concatenate([got1[g, pair[0]], got1[g, pair[1]]], axis=1), TOP_T1)

    for p in range(2):

        def load(g, total):
            value = both_of(g, pairs[p])
            moved[g] = value
            return total + value

        scale_into_x(lax.fori_loop(0, groups, load, zeros), p)

    def first_layer_of(which, rest):
        for i in which:
            for b in range(4):
                got("d", b, i)

        def one(p, carry):
            first_some([xs[i] for i in which], rest, p)
            return carry

        lax.fori_loop(0, 2, one, 0)

    first_layer_of((0, 1), False)
    pieces_3()
    weights_6(1)
    first_layer_of((2,), False)
    weights_6(2)
    weights_6(3)
    for k in range(4):
        got("d", 4, k)
    for b in range(1, 4):
        got("m", b)
    first_layer_of((), True)
    first_layer_of((3,), False)
    for p, (first, last) in enumerate(pairs):
        second_by_parts(p)

        def update(g, carry):
            value = both_of(g, pairs[p]) * growth(g)
            energy[g, first + 1] = value[:, :half]
            energy[g, last + 1] = value[:, half:]
            if p == 0:
                code = encode(value, TOP_E1)
                edge_out[0, g] = code[:, :half]
                edge_out[1, g] = code[:, half:]
            return carry

        lax.fori_loop(0, groups, update, 0, unroll=2)
        if p == 0:
            send_edges(0)

    for p in (1, 0):

        def pack(g, block):
            for i in range(2):
                at = g * 2 + i
                turned = pltpu.roll(energy[g, pairs[p][i] + 1], (at - edge_lane + half) % half, 1)
                block = jnp.where(lane == at, turned, block)
            return block

        col_out[p] = lax.fori_loop(0, groups, pack, thin, unroll=4)
        col_copies[p].start()
        if p == 1:
            send_edges(1)

    west_side = cb.astype(jnp.float32)

    def my_half(line):
        return jnp.where(cb == 0, line[:, :half], line[:, half:])


    def fill(present, copies_in, slot, row):
        @pl.when(present)
        def _():
            for c in copies_in:
                c.wait_recv()

            def some(g, carry):
                energy[g, row] = decode(edge_in[slot, g], TOP_E1)
                return carry

            lax.fori_loop(0, groups, some, 0)

        @pl.when(jnp.logical_not(present))
        def _():
            def some(g, carry):
                energy[g, row] = thin
                return carry

            lax.fori_loop(0, groups, some, 0)

    for n, pair in enumerate(pairs[::-1]):
        col_copies[1 - n].wait_recv()
        if n == 1:
            fill(has_up, edge_copies[1], 0, 0)
            fill(has_down, edge_copies[0], 1, 5)

        def second(g, total):
            coef = [coef_all[g, i] for i in range(7)]
            done = []
            for i, r in enumerate(pair):
                row = pl.ds(rb * 4 + r, 1)
                side = pltpu.roll(col_in[1 - n], (edge_lane - (g * 2 + i) + half) % half, 1)
                done.append(
                    transport_row(
                        energy[g, r], energy[g, r + 1], energy[g, r + 2], side * west_side, side * (1.0 - west_side),
                        coef, my_half(dx[row, :]), my_half(dy[row, :]), my_half(land[row, :]).astype(jnp.float32),
                    )
                )
            value = jnp.concatenate(done, axis=1)
            moved[g] = value
            return total + value

        scale_into_x(lax.fori_loop(0, groups, second, zeros, unroll=2), n)

        def halves(i, carry):
            first_half(i, n)
            return carry

        lax.fori_loop(0, 2, halves, 0)
        s_buf[...] = second_part(0, 9, n)

        def finish(k):
            g = (f + k) % 16
            code = encode(moved[g] * growth(g), TOP_E2)
            codes2[g, n * 2] = code[:, :half]
            codes2[g, n * 2 + 1] = code[:, half:]

        def finish_and_send(k, carry):
            finish(k)
            g = (f + k) % 16
            two = pl.ds(n * 2, 2)
            remote(codes2.at[g, two], got2.at[rb * 2 + cb, two], b_send.at[n, k], b_recv.at[n, k], at_freq(g)).start()
            return carry

        lax.fori_loop(1, groups, finish_and_send, 0, unroll=3)
        finish(0)

    own_back = pltpu.make_async_copy(codes2.at[f], got2.at[rb * 2 + cb], local_sem.at[0])
    own_back.start()

    def await_back(k, carry):
        g = (f + 16 - k) % 16
        b, c = block_of(g)
        for n in range(2):
            two = pl.ds(n * 2, 2)
            remote(codes2.at[0, two], got2.at[b * 2 + c, two], b_send.at[n, k], b_recv.at[n, k], at_freq(g)).wait_recv()
        put(b * 2 + c).start()
        return carry

    def put(n):
        return pltpu.make_async_copy(got2.at[n], out.at[n], store_sem.at[n])

    own_back.wait()
    put(rb * 2 + cb).start()
    lax.fori_loop(1, groups, await_back, 0)

    for c in z_copies + t_copies + list(copies.values()):
        c.wait_send()

    def sent(k, carry):
        for n in range(2):
            two = pl.ds(n * 2, 2)
            remote(codes2.at[0, two], got2.at[0, two], b_send.at[n, k], b_recv.at[n, k], partner).wait_send()
        return carry

    lax.fori_loop(1, groups, sent, 0)

    def sent_first(i, carry):
        first_copy(i).wait_send()
        put(i).wait()
        return carry

    lax.fori_loop(1, 16, sent_first, 0)
    put(0).wait()
    for c in col_copies:
        c.wait_send()
    pl.when(s > 0)(to_above.wait_send)
    pl.when(s < 15)(to_below.wait_send)
    for part in range(2):
        pl.when(has_up)(edge_copies[0][part].wait_send)
        pl.when(has_down)(edge_copies[1][part].wait_send)


def turn_back(codes_in, out, codes, lines_out, in_sem, out_sem):
    chans = out.shape[0]
    half = codes.shape[-1]
    slot = (2, 0, 1, 3)
    come = [pltpu.make_async_copy(codes_in.at[pl.ds(i * 2, 2)], codes.at[i], in_sem.at[i]) for i in range(4)]
    leave = [
        pltpu.make_async_copy(lines_out.at[i], out.at[:, pl.ds(i * 8, 8), :], out_sem.at[i]) for i in range(4)
    ]
    for c in come:
        c.start()
    for i in range(4):
        come[i].wait()
        for c in range(chans // 8):
            part = pl.ds(c * 8, 8)
            for side in range(2):
                lines = [decode(codes[i, n, side, slot[r], part, :], TOP_E2)[None] for n in range(2) for r in range(4)]
                turned = jnp.swapaxes(jnp.concatenate(lines, axis=0), 0, 1)
                lines_out[i, part, :, side * half : (side + 1) * half] = turned
        leave[i].start()
    for c in leave:
        c.wait()


def body(spectrum, land_sea, courant, refract, depth_dx, depth_dy, w_in, w_out):
    freqs, dirs, rows, cols = spectrum.shape
    chans = freqs * dirs
    half = cols // 2
    angles = (np.arange(DIRS, dtype=np.float32) + np.float32(0.5)) * np.float32(2.0 * math.pi / DIRS)
    cos_table = np.ascontiguousarray(np.broadcast_to(np.tile(np.cos(angles), freqs)[:, None], (chans, cols)))
    sin_table = np.ascontiguousarray(np.broadcast_to(np.tile(np.sin(angles), freqs)[:, None], (chans, cols)))
    anywhere = pl.BlockSpec(memory_space=pl.ANY)
    smem = pl.BlockSpec(memory_space=pltpu.SMEM)
    dma = pltpu.SemaphoreType.DMA
    i16, f32, b16 = jnp.int16, jnp.float32, jnp.bfloat16
    back = pl.pallas_call(
        kernel,
        out_shape=jax.ShapeDtypeStruct((16, 4, chans, half), i16),
        in_specs=[anywhere] * 4 + [smem] * 2 + [anywhere] * 4,
        out_specs=anywhere,
        scratch_shapes=[
            pltpu.VMEM((chans, rows, cols), f32),
            pltpu.VMEM((rows, cols), f32),
            pltpu.VMEM((rows, cols), f32),
            pltpu.VMEM((rows, cols), jnp.int32),
            pltpu.VMEM((chans, cols), f32),
            pltpu.VMEM((chans, cols), f32),
            pltpu.VMEM((9, 128, 128), b16),
            pltpu.VMEM((128, 9 * 128), b16),
            pltpu.VMEM((rows + 2, chans, cols), f32),
            pltpu.VMEM((8, cols), f32),
            pltpu.VMEM((9, 128, 128), b16),
            pltpu.VMEM((2, 16, 9, 128, 128), b16),
            pltpu.VMEM((16, 4, chans, half), i16),
            pltpu.VMEM((16, 4, chans, half), i16),
            pltpu.VMEM((16, 4, chans, half), i16),
            pltpu.VMEM((16, 4, chans, half), i16),
            pltpu.VMEM((16, 8, cols), f32),
            pltpu.VMEM((2, 16, chans, half), i16),
            pltpu.VMEM((2, 16, chans, half), i16),
            pltpu.VMEM((2, chans, half), f32),
            pltpu.VMEM((2, chans, half), f32),
            pltpu.VMEM((16, 6, chans, half), f32),
            pltpu.VMEM((16, chans, cols), f32),
            pltpu.VMEM((2, 16 * chans, cols), b16),
            pltpu.VMEM((2, 2048, cols), b16),
            pltpu.VMEM((16 * chans, cols), f32),
            pltpu.VMEM((7, chans, cols), f32),
            pltpu.VMEM((16, 7, chans, half), f32),
            dma((4,)), dma((4,)), dma((4,)), dma((4,)), dma((5, 4)), dma((5, 4)), dma((5, 4)), dma((5, 4)),
            dma((16,)), dma((16,)), dma((16,)), dma((16,)), dma((2, 2)), dma((2, 2)), dma((2, 16)), dma((2, 16)),
            dma((2,)), dma((2,)), dma((2,)), dma((2,)), dma((4,)), dma((4,)), dma((4,)), dma((4,)),
            dma((1,)), dma((8,)), dma((16,)),
        ],
        compiler_params=pltpu.CompilerParams(
            collective_id=0, has_side_effects=True, vmem_limit_bytes=60 * 1024 * 1024
        ),
    )(
        spectrum.reshape(chans, rows, cols), depth_dx, depth_dy, land_sea, courant, refract, cos_table, sin_table,
        w_in.reshape(9, 128, 128), w_out,
    )
    result = pl.pallas_call(
        turn_back,
        out_shape=jax.ShapeDtypeStruct((chans, rows, cols), f32),
        in_specs=[anywhere],
        out_specs=anywhere,
        scratch_shapes=[
            pltpu.VMEM((4, 2, 2, 4, chans, half), i16),
            pltpu.VMEM((4, chans, 8, cols), f32),
            dma((4,)),
            dma((4,)),
        ],
    )(back.reshape(8, 2, 4, chans, half))
    return result.reshape(freqs, dirs, rows, cols)


def solution(mesh):
    placed = (
        P("freq", None, "space", None),
        P("space", None),
        P("freq"),
        P("freq"),
        P("space", None),
        P("space", None),
        P(None, "freq"),
        P("freq", None),
    )
    return jax.shard_map(
        body, mesh=mesh, in_specs=placed, out_specs=P("freq", None, "space", None), check_vma=False
    )
```
